128 devices in a mesh: dp: 8 (over y, core), pipe: 4 (over x), tensor: 4 (over z).
Axes of the slice: x: 4, y: 4, z: 4, core: 2. Of those that a mesh axis runs over, the one named last changes fastest.
Arguments:
- query_states: bfloat16 [16, 512, 1024], P('dp'), may hold values from -6 to 6
- doc_states: bfloat16 [16, 512, 1024], P('dp'), may hold values from -6 to 6
- query_len: int32 [16], P('dp'), may hold values from 64 to 512
- doc_len: int32 [16], P('dp'), may hold values from 64 to 512
- doc_order: int32 [8, 2], P('dp'), may hold values from 0 to 1, each once within a row
- w_qkv: bfloat16 [4, 3, 1024, 1024], P('pipe', None, None, 'tensor'), may hold values from -0.1875 to 0.1875
- w_out: bfloat16 [4, 1024, 1024], P('pipe', 'tensor'), may hold values from -0.1875 to 0.1875
- w_up: bfloat16 [4, 1024, 4096], P('pipe', None, 'tensor'), may hold values from -0.1875 to 0.1875
- w_down: bfloat16 [4, 4096, 1024], P('pipe', 'tensor'), may hold values from -0.09375 to 0.09375
- gain_attn: float32 [4, 1024], P('pipe'), may hold values from 0.1 to 1.9
- gain_mlp: float32 [4, 1024], P('pipe'), may hold values from 0.1 to 1.9
Outputs:
- query_vectors: bfloat16 [16, 1024], P('dp', ('pipe', 'tensor'))
- document_vectors: bfloat16 [16, 1024], P('dp', ('pipe', 'tensor'))
- pair_loss: float32 [16], P('dp')
The draws below stay inside these ranges and needn't reach their ends.
Inputs may be any that keep to these rules, and one draw needn't show every extreme that they name: `doc_order`: each row holds every number of 0 to 1 once.
All inputs are finite; a program needn't handle non-finite values.
Results may differ from the reference program's by a relative error of at most 0.035.
Values may be sent and summed in bfloat16 or wider, within the bound.
A program may use at most 192 MiB of HBM per device.

```python
import math
import jax
import jax.numpy as jnp
from jax import lax

D = 1024
HEADS = 16
FF = 4096
S = 512
PAIRS_DEV = 2
LAYERS = 4
QUERIES = 16
DOCS = 16
N_DP = 8
N_TENSOR = 4


def set_ends(values, stream_key, low, high):
    longest = values.shape.index(max(values.shape))
    spots = []
    for shift in (0, 1):
        where = [jax.random.randint(jax.random.fold_in(stream_key, axis), (), 0, length) for axis, length in enumerate(values.shape)]
        where[longest] = (where[longest] + shift) % values.shape[longest]
        spots.append(tuple(where))
    return values.at[spots[0]].set(low).at[spots[1]].set(high)


def levels(stream_key, shape, split, low, top_value):
    loudness = 1.0
    for dim, parts in split:
        heights = jax.random.uniform(jax.random.fold_in(jax.random.fold_in(stream_key, 6), dim), (parts,), jnp.float32, low / len(split), top_value / len(split))
        loudness = loudness * jnp.repeat(jnp.exp(heights), shape[dim] // parts).reshape((-1,) + (1,) * (len(shape) - 1 - dim))
    return loudness


def centred(key, dims, spread, limit, split=(), kind=jnp.bfloat16):
    entries = spread * jax.random.normal(key, dims, jnp.float32)
    if split:
        entries = entries * levels(key, dims, split, -0.22, 0.18)
    return jnp.clip(entries, -limit, limit).astype(kind)


def setup_inputs(seed: int = 0) -> dict:
    arg_keys = jax.random.split(jax.random.key(seed), 12)
    query_states = centred(arg_keys[0], (QUERIES, S, D), 1.0, 6.0, ((0, 8),))
    doc_states = centred(arg_keys[1], (DOCS, S, D), 1.0, 6.0, ((0, 8),))
    query_len = set_ends(jax.random.randint(arg_keys[2], (QUERIES,), S // 8, S + 1), jax.random.fold_in(arg_keys[2], 1), S // 8, S).astype(jnp.int32)
    doc_len = set_ends(jax.random.randint(arg_keys[3], (DOCS,), S // 8, S + 1), jax.random.fold_in(arg_keys[3], 1), S // 8, S).astype(jnp.int32)
    doc_order = jax.vmap(lambda own: jax.random.permutation(own, PAIRS_DEV))(jax.random.split(arg_keys[4], N_DP)).reshape((N_DP, PAIRS_DEV)).astype(jnp.int32)
    w_qkv = centred(arg_keys[5], (LAYERS, 3, D, D), D ** -0.5, 0.1875, ((0, 4), (3, 4)))
    w_out = centred(arg_keys[6], (LAYERS, D, D), D ** -0.5, 0.1875, ((0, 4), (1, 4)))
    w_up = centred(arg_keys[7], (LAYERS, D, FF), D ** -0.5, 0.1875, ((0, 4), (2, 4)))
    w_down = centred(arg_keys[8], (LAYERS, FF, D), FF ** -0.5, 0.09375, ((0, 4), (1, 4)))
    gain_attn = jnp.clip(1.0 + 0.18 * jax.random.normal(arg_keys[9], (LAYERS, D), jnp.float32), 0.1, 1.9)
    gain_mlp = jnp.clip(1.0 + 0.18 * jax.random.normal(arg_keys[10], (LAYERS, D), jnp.float32), 0.1, 1.9)
    return {"query_states": query_states, "doc_states": doc_states, "query_len": query_len, "doc_len": doc_len, "doc_order": doc_order, "w_qkv": w_qkv, "w_out": w_out, "w_up": w_up, "w_down": w_down, "gain_attn": gain_attn, "gain_mlp": gain_mlp}


SOFTMAX_TEMPER = 0.05
EPSILON = 1e-06
LAYER_EPSILON = 1e-12

def norm_rows(values_in, gain_row):
    row_mean = lax.optimization_barrier(jnp.mean(values_in, axis=-1, keepdims=True))
    centered = values_in - row_mean
    variance = lax.optimization_barrier(jnp.mean(centered * centered, axis=-1, keepdims=True))
    return centered * lax.rsqrt(variance + LAYER_EPSILON) * gain_row

def group_sum(left_side, right_side):
    row_total = left_side.shape[0]
    group_width = left_side.shape[1] // N_TENSOR
    left_parts = left_side.reshape(row_total, N_TENSOR, group_width).astype(jnp.float32)
    right_parts = right_side.reshape(N_TENSOR, group_width, right_side.shape[1]).astype(jnp.float32)
    partials = jnp.einsum('sgk,gkd->gsd', left_parts, right_parts)
    rounded = lax.optimization_barrier(partials.astype(jnp.bfloat16))
    return lax.optimization_barrier(jnp.sum(rounded.astype(jnp.float32), axis=0))

def encode_layer(hidden, valid_keys, w_qkv, w_out, w_up, w_down, gain_attn, gain_mlp):
    head_width = D // HEADS
    slot_count = hidden.shape[0]
    inv_sqrt = 1.0 / math.sqrt(head_width)
    query_rows = (jnp.dot(hidden, w_qkv[0], preferred_element_type=jnp.float32) * inv_sqrt).astype(jnp.bfloat16)
    key_rows = jnp.dot(hidden, w_qkv[1], preferred_element_type=jnp.float32).astype(jnp.bfloat16)
    value_rows = jnp.dot(hidden, w_qkv[2], preferred_element_type=jnp.float32).astype(jnp.bfloat16)
    query_heads = query_rows.reshape(slot_count, HEADS, head_width).astype(jnp.float32)
    key_heads = key_rows.reshape(slot_count, HEADS, head_width).astype(jnp.float32)
    value_heads = value_rows.reshape(slot_count, HEADS, head_width).astype(jnp.float32)
    scores = jnp.einsum('qhe,khe->hqk', query_heads, key_heads)
    exp_scores = jnp.where(valid_keys[None, None, :], jnp.exp(scores), 0.0)
    attention = (exp_scores / lax.optimization_barrier(jnp.sum(exp_scores, axis=-1, keepdims=True))).astype(jnp.bfloat16)
    context = jnp.einsum('hqk,khe->qhe', attention.astype(jnp.float32), value_heads)
    context = context.astype(jnp.bfloat16).reshape(slot_count, D)
    mixed = norm_rows(hidden.astype(jnp.float32) + group_sum(context, w_out), gain_attn).astype(jnp.bfloat16)
    upward = jnp.dot(mixed, w_up, preferred_element_type=jnp.float32)
    activated = jax.nn.gelu(upward, approximate=False).astype(jnp.bfloat16)
    return norm_rows(mixed.astype(jnp.float32) + group_sum(activated, w_down), gain_mlp).astype(jnp.bfloat16)

def reference(query_states, doc_states, query_len, doc_len, doc_order, w_qkv, w_out, w_up, w_down, gain_attn, gain_mlp):

    def embed_sequence(item):
        states, seq_length = item
        positions = jnp.arange(states.shape[0], dtype=jnp.int32)
        valid_keys = positions < seq_length
        hidden = states
        for layer_index in range(w_qkv.shape[0]):
            hidden = encode_layer(hidden, valid_keys, w_qkv[layer_index], w_out[layer_index], w_up[layer_index], w_down[layer_index], gain_attn[layer_index], gain_mlp[layer_index])
        summed = lax.optimization_barrier(jnp.sum(jnp.where(valid_keys[:, None], hidden.astype(jnp.float32), 0.0), axis=0))
        pooled = summed / seq_length.astype(jnp.float32)
        return (pooled * lax.rsqrt(jnp.sum(pooled * pooled) + EPSILON)).astype(jnp.bfloat16)
    query_vectors = lax.map(embed_sequence, (query_states, query_len))
    document_vectors = lax.map(embed_sequence, (doc_states, doc_len))
    complete_scores = jnp.dot(query_vectors, document_vectors.T, preferred_element_type=jnp.float32) / SOFTMAX_TEMPER
    exp_total = lax.optimization_barrier(jnp.sum(jnp.exp(complete_scores), axis=1))
    shard_base = jnp.arange(N_DP, dtype=jnp.int32)[:, None] * PAIRS_DEV
    positive_index = (shard_base + doc_order.astype(jnp.int32)).reshape(-1)
    positive_score = jnp.take_along_axis(complete_scores, positive_index[:, None], axis=1)[:, 0]
    pair_loss = jnp.log(exp_total) - positive_score
    return (query_vectors, document_vectors, pair_loss)
```

```python
import jax
import jax.numpy as jnp
from jax import lax
from jax.experimental import pallas as pl
from jax.experimental.pallas import tpu as pltpu
from jax.sharding import PartitionSpec as P

S = 512
D = 1024
G = 256
HALF = 256
BF = jnp.bfloat16
F32 = jnp.float32
LOG2E = 1.4426950408889634
VSCALE = 2.0**-14
SQRT_HALF = 0.7071067811865476
MESH = pl.DeviceIdType.MESH
ARRAYS = ("qkv", "out", "up", "down")


def dot(a, b):
    return jnp.dot(a, b, preferred_element_type=F32)


def norm_rows(x, gain):
    mean = jnp.mean(x, axis=-1, keepdims=True)
    centered = x - mean
    variance = jnp.mean(centered * centered, axis=-1, keepdims=True)
    return centered * lax.rsqrt(variance + 1e-12) * gain


def gelu(u):
    return 0.5 * u * (1.0 + lax.erf(u * SQRT_HALF))


class Sems:
    def __init__(self, send, recv):
        self.send, self.recv, self.used = send, recv, 0

    def remote(self, src, dst, device):
        i = self.used
        self.used += 1
        return pltpu.make_async_remote_copy(
            src_ref=src, dst_ref=dst, send_sem=self.send.at[i], recv_sem=self.recv.at[i], device_id=device, device_id_type=MESH
        )


N_SEMS = 36


def kernel(
    states_q, states_d, qlen, dlen, order, w_qkv, w_out, w_up, w_down, gain_attn, gain_mlp,
    out_q, out_d, out_loss,
    b_qkv, b_out, b_up, b_down, h, hout, qkv, qm, km, kt, vm, cf, ctx, acc, mixed, act, qtab, dtab, tile,
    send, recv, local, h_send, h_recv, t1_send, t1_recv, t2_send, t2_recv, t3_send, t3_recv,
):
    dp, pipe, z = lax.axis_index("dp"), lax.axis_index("pipe"), lax.axis_index("tensor")
    core = lax.rem(dp, 2)
    first = 1 - (pipe + 3) // 4

    def at(dp_=dp, pipe_=pipe, z_=z):
        return (dp_, pipe_, z_)

    up_z, down_z = at(z_=lax.rem(z + 1, 4)), at(z_=lax.rem(z + 3, 4))
    sibling = at(dp_=dp + 1 - 2 * core)

    barrier = pltpu.get_barrier_semaphore()
    for k in range(1, 8):
        pl.semaphore_signal(barrier, inc=1, device_id=at(dp_=lax.rem(dp + k, 8)), device_id_type=MESH)
    for k in range(1, 4):
        pl.semaphore_signal(barrier, inc=1, device_id=at(pipe_=lax.rem(pipe + k, 4)), device_id_type=MESH)
        pl.semaphore_signal(barrier, inc=1, device_id=at(z_=lax.rem(z + k, 4)), device_id_type=MESH)

    own = {"qkv": w_qkv, "out": w_out, "up": w_up, "down": w_down}
    full = {"qkv": b_qkv, "out": b_out, "up": b_up, "down": b_down}
    depth = {"qkv": 1024, "out": 256, "up": 1024, "down": 1024}

    def rows_of(name, ref, which):
        n = depth[name] // 4
        if which == "a":
            start, size = core * 2 * n, n
        elif which == "b":
            start, size = core * 2 * n + n, n
        elif which == "all":
            start, size = core * 2 * n, 2 * n
        else:
            start, size = (1 - core) * 2 * n, 2 * n
        sl = pl.ds(pl.multiple_of(start, n), size)
        return ref.at[:, sl, :] if name == "qkv" else ref.at[sl, :]

    sems = Sems(send, recv)
    hop1, hop2, d2d = {}, {}, {}
    for name in ARRAYS:
        for part in ("a", "b"):
            src = rows_of(name, own[name].at[0], part)
            hop1[name, 1, part] = sems.remote(src, rows_of(name, full[name].at[1], part), up_z)
            hop1[name, 2, part] = sems.remote(src, rows_of(name, full[name].at[2], part), down_z)
        hop2[name, "a"] = sems.remote(rows_of(name, full[name].at[1], "a"), rows_of(name, full[name].at[3], "a"), up_z)
        hop2[name, "b"] = sems.remote(rows_of(name, full[name].at[2], "b"), rows_of(name, full[name].at[3], "b"), down_z)
        for slot in (1, 2, 3):
            mine = rows_of(name, full[name].at[slot], "all")
            d2d[name, slot] = sems.remote(mine, mine, sibling)
    loads = {name: pltpu.make_async_copy(own[name].at[0], full[name].at[0], local.at[i]) for i, name in enumerate(ARRAYS)}

    def start_own(names):
        for name in names:
            for part in ("a", "b"):
                hop1[name, 1, "a" if part == "a" else "b"].start()
                hop1[name, 2, "b" if part == "a" else "a"].start()

    def forward(names):
        for name in names:
            hop1[name, 1, "a"].wait_recv()
            hop2[name, "a"].start()
            hop1[name, 2, "b"].wait_recv()
            hop2[name, "b"].start()

    def near(names):
        for name in names:
            hop1[name, 1, "b"].wait_recv()
            d2d[name, 1].start()
            hop1[name, 2, "a"].wait_recv()
            d2d[name, 2].start()
        for name in names:
            for slot in (1, 2):
                d2d[name, slot].wait_recv()

    def far(names):
        for name in names:
            hop2[name, "a"].wait_recv()
            hop2[name, "b"].wait_recv()
            d2d[name, 3].start()
        for name in names:
            d2d[name, 3].wait_recv()

    for name in ARRAYS:
        loads[name].start()
    gains = [pltpu.make_async_copy(gain_attn, tile.at[pl.ds(0, 1)], local.at[4]), pltpu.make_async_copy(gain_mlp, tile.at[pl.ds(8, 1)], local.at[5])]
    for g in gains:
        g.start()

    pl.semaphore_wait(barrier, 13)
    ATT, MLP = ("qkv", "out"), ("up", "down")
    start_own(ATT)

    z_low = lax.rem(z, 2)

    @pl.when((first == 1) & (z < 2))
    def _():
        c = pltpu.make_async_copy(states_q.at[z_low], h, local.at[6])
        c.start()
        c.wait()

    @pl.when((first == 1) & (z >= 2))
    def _():
        c = pltpu.make_async_copy(states_d.at[z_low], h, local.at[6])
        c.start()
        c.wait()

    @pl.when(first == 0)
    def _():
        forward(ATT)
        start_own(MLP)
        near(ATT)
        far(ATT)
        forward(MLP)
        near(MLP)
        far(MLP)

    for name in ARRAYS:
        loads[name].wait()
    for g in gains:
        g.wait()

    nblk = S // HALF

    def hop_x(r):
        rows = pl.ds(r * HALF, HALF)
        return pltpu.make_async_remote_copy(
            src_ref=hout.at[rows], dst_ref=h.at[rows], send_sem=h_send.at[r], recv_sem=h_recv.at[r],
            device_id=at(pipe_=lax.rem(pipe + 1, 4)), device_id_type=MESH,
        )

    @pl.when(first == 0)
    def _():
        for r in range(nblk):
            hop_x(r).wait_recv()

    length = jnp.where(z == 0, qlen[0], jnp.where(z == 1, qlen[1], jnp.where(z == 2, dlen[0], dlen[1])))
    lane = lax.broadcasted_iota(jnp.int32, (1, G), 1)
    head = lane // 64
    bias = jnp.where(lax.broadcasted_iota(jnp.int32, (1, S), 1) < length, 0.0, -1e30).astype(BF)
    krow = lax.broadcasted_iota(jnp.int32, (G, 1), 0)
    one, zero = jnp.ones((), BF), jnp.zeros((), BF)

    @pl.loop(0, 4)
    def _(j):
        @pl.when((first == 1) & (j == 1))
        def _():
            forward(ATT)
            start_own(MLP)
            near(ATT)

        @pl.when((first == 1) & (j == 3))
        def _():
            far(ATT)

        @pl.loop(0, 3)
        def _(i):
            scale = jnp.where(i == 0, 0.125 * LOG2E, jnp.where(i == 2, VSCALE, 1.0)).astype(F32)
            qkv[i] = (dot(h[...], b_qkv[j, i]) * scale).astype(BF)

        kt[...] = qkv[1].T
        for hd in range(4):
            nxt = (hd + 1) % 4
            mine, other, mark = head == hd, head == nxt, lane == nxt * 64
            qm[hd] = jnp.where(mine, qkv[0], jnp.where(mark, one, zero))
            km[hd] = jnp.where(krow == nxt * 64, bias, kt[...])
            vm[hd] = jnp.where(mine, qkv[2], jnp.where(other, one, zero))
        for hd in range(4):
            mine = head == hd
            for r in range(2):
                rows = slice(r * 256, (r + 1) * 256)
                p = jnp.exp2(dot(qm[hd, rows, :], km[hd])).astype(BF)
                o = dot(p, vm[hd])
                total = pltpu.roll(o, 192, 1)
                t = jnp.where(total > 2.0**60, 2.0**-64, 1.0).astype(F32)
                c = (o * t) * (1.0 / (total * t)) * (1.0 / VSCALE)
                cf[rows, :] = jnp.where(mine, c, cf[rows, :] if hd else c)
        ctx[:, pl.ds(pl.multiple_of(j * G, G), G)] = cf[...].astype(BF)

    @pl.loop(0, 4)
    def _(n):
        cs = pl.ds(pl.multiple_of(n * 256, 256), 256)
        acc[:, cs] = sum(dot(ctx[:, j * G : (j + 1) * G], b_out[j, :, cs]) for j in range(4))

    @pl.loop(0, 4)
    def _(r):
        for q in range(4):
            rows = pl.ds(pl.multiple_of(r * 128 + q * 32, 32), 32)
            mixed[rows, :] = norm_rows(h[rows, :].astype(F32) + acc[rows, :], tile[0:1, :]).astype(BF)

    @pl.loop(0, 4 * nblk)
    def _(i):
        j = first * (i // nblk) + (1 - first) * lax.rem(i, 4)
        r = first * lax.rem(i, nblk) + (1 - first) * (i // 4)

        @pl.when((first == 1) & (i == nblk))
        def _():
            forward(MLP)
            near(MLP)

        @pl.when((first == 1) & (i == 3 * nblk))
        def _():
            far(MLP)

        rows = pl.ds(pl.multiple_of(r * HALF, HALF), HALF)

        @pl.loop(0, 4)
        def _(n):
            cs = pl.ds(pl.multiple_of(n * 256, 256), 256)
            act[:, cs] = gelu(dot(mixed[rows, :], b_up[j, :, cs])).astype(BF)

        @pl.loop(0, 4)
        def _(n):
            cs = pl.ds(pl.multiple_of(n * 256, 256), 256)
            part = dot(act[...], b_down[j, :, cs])
            acc[rows, cs] = jnp.where(j == 0, part, acc[rows, cs] + part)

        @pl.when(j == 3)
        def _():
            @pl.loop(0, HALF // 64)
            def _(q):
                for u in range(2):
                    rr = pl.ds(pl.multiple_of(r * HALF + q * 64 + u * 32, 32), 32)
                    hout[rr, :] = norm_rows(mixed[rr, :].astype(F32) + acc[rr, :], tile[8:9, :]).astype(BF)

            for rs in range(nblk):

                @pl.when((pipe < 3) & (r == rs))
                def _():
                    hop_x(rs).start()

    def t1(k):
        return pltpu.make_async_remote_copy(
            src_ref=dtab.at[z_low, dp], dst_ref=dtab.at[z_low, dp], send_sem=t1_send.at[k - 1], recv_sem=t1_recv.at[k - 1],
            device_id=at(dp_=lax.rem(dp + k, 8)), device_id_type=MESH,
        )

    def t1_in(k):
        there = lax.rem(dp + 8 - k, 8)
        return pltpu.make_async_remote_copy(
            src_ref=dtab.at[z_low, there], dst_ref=dtab.at[z_low, there], send_sem=t1_send.at[k - 1], recv_sem=t1_recv.at[k - 1],
            device_id=at(dp_=lax.rem(dp + k, 8)), device_id_type=MESH,
        )

    def t2(tab, slot, k):
        return pltpu.make_async_remote_copy(
            src_ref=tab.at[slot], dst_ref=tab.at[slot], send_sem=t2_send.at[k - 1], recv_sem=t2_recv.at[k - 1],
            device_id=at(z_=lax.rem(z + k, 4)), device_id_type=MESH,
        )

    def t3(tab, i, k):
        return pltpu.make_async_remote_copy(
            src_ref=tab, dst_ref=tab, send_sem=t3_send.at[i, k], recv_sem=t3_recv.at[i], device_id=at(pipe_=k), device_id_type=MESH
        )

    @pl.when(pipe < 3)
    def _():
        t3(qtab, 0, 0).wait_recv()
        t3(dtab, 1, 0).wait_recv()

    @pl.when(pipe == 3)
    def _():
        acc[0:8, :] = jnp.zeros((8, D), F32)

        @pl.loop(0, 16)
        def _(r):
            rows = pl.ds(pl.multiple_of(r * 32, 32), 32)
            keep = lax.broadcasted_iota(jnp.int32, (32, 1), 0) + r * 32 < length
            x = jnp.where(keep, hout[rows, :].astype(F32), 0.0)
            acc[0:8, :] += x[0:8] + x[8:16] + x[16:24] + x[24:32]

        pooled = jnp.sum(acc[0:8, :], axis=0, keepdims=True) / length.astype(F32)
        emb = pooled * lax.rsqrt(jnp.sum(pooled * pooled, axis=-1, keepdims=True) + 1e-6)
        emb = emb.astype(BF).astype(F32)

        @pl.when(z < 2)
        def _():
            for k in range(8):
                qtab[z_low, k : k + 1, :] = emb[:, k * 128 : (k + 1) * 128]

        @pl.when(z >= 2)
        def _():
            for k in range(8):
                dtab[z_low, dp, k : k + 1, :] = emb[:, k * 128 : (k + 1) * 128]
            for k in range(1, 8):
                t1(k).start()
            for k in range(1, 8):
                t1_in(k).wait_recv()
            for k in range(1, 4):
                t2(dtab, z_low, k).start()

        @pl.when(z < 2)
        def _():
            for k in range(1, 4):
                t2(qtab, z_low, k).start()

        for k in range(1, 4):
            there = lax.rem(z + 4 - k, 4)

            @pl.when(there < 2)
            def _():
                t2(qtab, lax.rem(there, 2), k).wait_recv()

            @pl.when(there >= 2)
            def _():
                t2(dtab, lax.rem(there, 2), k).wait_recv()

        for k in range(3):
            t3(qtab, 0, k).start()
            t3(dtab, 1, k).start()

    doc_dp = lax.broadcasted_iota(jnp.int32, (8, 1), 0)
    for i in range(2):
        total, positive = jnp.zeros((1, 1), F32), jnp.zeros((1, 1), F32)
        for s in range(2):
            prod = dtab[s] * qtab[i][None]
            score = jnp.sum(jnp.sum(prod, axis=1), axis=1, keepdims=True) / 0.05
            total += jnp.sum(jnp.exp(score), axis=0, keepdims=True)
            hit = (doc_dp == dp) & (order[0, i] == s)
            positive += jnp.sum(jnp.where(hit, score, 0.0), axis=0, keepdims=True)
        out_loss[i : i + 1, :] = jnp.broadcast_to(jnp.log(total) - positive, (1, 128))
    piece = pipe * 4 + z
    row, side = piece // 2, lax.rem(piece, 2)
    for i in range(2):
        qrow = qtab[i, pl.ds(row, 1), :]
        out_q[i : i + 1, :] = jnp.where(side == 0, qrow, pltpu.roll(qrow, 64, 1))[:, :64].astype(BF)
        drow = dtab[i, dp, pl.ds(row, 1), :]
        out_d[i : i + 1, :] = jnp.where(side == 0, drow, pltpu.roll(drow, 64, 1))[:, :64].astype(BF)

    for copy in [*hop1.values(), *hop2.values(), *d2d.values()]:
        copy.wait_send()

    @pl.when(pipe < 3)
    def _():
        for r in range(nblk):
            hop_x(r).wait_send()

    @pl.when(pipe == 3)
    def _():
        for k in range(3):
            t3(qtab, 0, k).wait_send()
            t3(dtab, 1, k).wait_send()

        @pl.when(z >= 2)
        def _():
            for k in range(1, 8):
                t1(k).wait_send()
            for k in range(1, 4):
                t2(dtab, z_low, k).wait_send()

        @pl.when(z < 2)
        def _():
            for k in range(1, 4):
                t2(qtab, z_low, k).wait_send()


def per_device(query_states, doc_states, query_len, doc_len, doc_order, w_qkv, w_out, w_up, w_down, gain_attn, gain_mlp):
    anyspace = pl.BlockSpec(memory_space=pl.ANY)
    smem = pl.BlockSpec(memory_space=pltpu.SMEM)
    vmem = pl.BlockSpec(memory_space=pltpu.VMEM)
    q, d, loss = pl.pallas_call(
        kernel,
        out_shape=(jax.ShapeDtypeStruct((2, 64), BF), jax.ShapeDtypeStruct((2, 64), BF), jax.ShapeDtypeStruct((2, 128), F32)),
        in_specs=[anyspace, anyspace, smem, smem, smem, *[anyspace] * 6],
        out_specs=(vmem, vmem, vmem),
        scratch_shapes=[
            pltpu.VMEM((4, 3, D, G), BF),
            pltpu.VMEM((4, G, D), BF),
            pltpu.VMEM((4, D, D), BF),
            pltpu.VMEM((4, D, D), BF),
            pltpu.VMEM((S, D), BF),
            pltpu.VMEM((S, D), BF),
            pltpu.VMEM((3, S, G), BF),
            pltpu.VMEM((4, S, G), BF),
            pltpu.VMEM((4, G, S), BF),
            pltpu.VMEM((G, S), BF),
            pltpu.VMEM((4, S, G), BF),
            pltpu.VMEM((S, G), F32),
            pltpu.VMEM((S, D), BF),
            pltpu.VMEM((S, D), F32),
            pltpu.VMEM((S, D), BF),
            pltpu.VMEM((HALF, D), BF),
            pltpu.VMEM((2, 8, 128), F32),
            pltpu.VMEM((2, 8, 8, 128), F32),
            pltpu.VMEM((16, D), F32),
            pltpu.SemaphoreType.DMA((N_SEMS,)),
            pltpu.SemaphoreType.DMA((N_SEMS,)),
            pltpu.SemaphoreType.DMA((8,)),
            pltpu.SemaphoreType.DMA((S // HALF,)),
            pltpu.SemaphoreType.DMA((S // HALF,)),
            pltpu.SemaphoreType.DMA((7,)),
            pltpu.SemaphoreType.DMA((7,)),
            pltpu.SemaphoreType.DMA((3,)),
            pltpu.SemaphoreType.DMA((3,)),
            pltpu.SemaphoreType.DMA((2, 3)),
            pltpu.SemaphoreType.DMA((2,)),
        ],
        compiler_params=pltpu.CompilerParams(collective_id=0, has_side_effects=True, vmem_limit_bytes=63 * 2**20),
        name="encode",
    )(query_states, doc_states, query_len, doc_len, doc_order, w_qkv, w_out, w_up, w_down, gain_attn, gain_mlp)
    return q, d, loss[:, 0]


def solution(mesh):
    in_specs = (
        P("dp", None, None),
        P("dp", None, None),
        P("dp"),
        P("dp"),
        P("dp", None),
        P("pipe", None, None, "tensor"),
        P("pipe", "tensor", None),
        P("pipe", None, "tensor"),
        P("pipe", "tensor", None),
        P("pipe", None),
        P("pipe", None),
    )
    out_specs = (P("dp", ("pipe", "tensor")), P("dp", ("pipe", "tensor")), P("dp"))
    return jax.shard_map(per_device, mesh=mesh, in_specs=in_specs, out_specs=out_specs, check_vma=False)
```

```python
import jax
import jax.numpy as jnp
from jax import lax
from jax.experimental import pallas as pl
from jax.experimental.pallas import tpu as pltpu
from jax.sharding import PartitionSpec as P

S = 512
D = 1024
G = 256
HALF = 256
BF = jnp.bfloat16
F32 = jnp.float32
LOG2E = 1.4426950408889634
VSCALE = 2.0**-14
SQRT_HALF = 0.7071067811865476
MESH = pl.DeviceIdType.MESH
ARRAYS = ("qkv", "out", "up", "down")
MLP = ("up", "down")
depth_half = {"qkv": 512, "out": 128, "up": 512, "down": 512}


def dot(a, b):
    return jnp.dot(a, b, preferred_element_type=F32)


def norm_rows(x, gain):
    mean = jnp.mean(x, axis=-1, keepdims=True)
    centered = x - mean
    variance = jnp.mean(centered * centered, axis=-1, keepdims=True)
    return centered * lax.rsqrt(variance + 1e-12) * gain


def gelu(u):
    return 0.5 * u * (1.0 + lax.erf(u * SQRT_HALF))


class Sems:
    def __init__(self, send, recv):
        self.send, self.recv, self.used = send, recv, 0

    def remote(self, src, dst, device):
        i = self.used
        self.used += 1
        return pltpu.make_async_remote_copy(
            src_ref=src, dst_ref=dst, send_sem=self.send.at[i], recv_sem=self.recv.at[i], device_id=device, device_id_type=MESH
        )


    def again(self, i, ref, device):
        return pltpu.make_async_remote_copy(
            src_ref=ref, dst_ref=ref, send_sem=self.send.at[i], recv_sem=self.recv.at[i], device_id=device, device_id_type=MESH
        )


N_SEMS = 60


def kernel(
    states_q, states_d, qlen, dlen, order, w_qkv, w_out, w_up, w_down, gain_attn, gain_mlp,
    out_q, out_d, out_loss,
    b_qkv, b_out, b_up, b_down, h, hout, qkv, qm, km, kt, vm, cf, ctx, acc, mixed, act, qtab, dtab, tile,
    send, recv, local, c_send, c_recv, h_send, h_recv, t1_send, t1_recv, t2_send, t2_recv, t3_send, t3_recv,
):
    dp, pipe, z = lax.axis_index("dp"), lax.axis_index("pipe"), lax.axis_index("tensor")
    core = lax.rem(dp, 2)
    first = 1 - (pipe + 3) // 4

    def at(dp_=dp, pipe_=pipe, z_=z):
        return (dp_, pipe_, z_)

    up_z, down_z = at(z_=lax.rem(z + 1, 4)), at(z_=lax.rem(z + 3, 4))
    sibling = at(dp_=dp + 1 - 2 * core)

    barrier = pltpu.get_barrier_semaphore()
    for k in range(1, 8):
        pl.semaphore_signal(barrier, inc=1, device_id=at(dp_=lax.rem(dp + k, 8)), device_id_type=MESH)
    for k in range(1, 4):
        pl.semaphore_signal(barrier, inc=1, device_id=at(pipe_=lax.rem(pipe + k, 4)), device_id_type=MESH)
        pl.semaphore_signal(barrier, inc=1, device_id=at(z_=lax.rem(z + k, 4)), device_id_type=MESH)

    y = dp // 2
    own = {"qkv": w_qkv, "out": w_out, "up": w_up, "down": w_down}
    full = {"qkv": b_qkv, "out": b_out, "up": b_up, "down": b_down}
    north, south = at(dp_=lax.rem(dp + 2, 8)), at(dp_=lax.rem(dp + 6, 8))

    def window(name, ref, start, size):
        sl = pl.ds(pl.multiple_of(start, 16), size)
        return ref.at[:, sl, :] if name == "qkv" else ref.at[sl, :]

    def quarter(k):
        return core * 512 + 128 + 96 * lax.rem(y + k + 4, 4)

    parts = {
        "qkv": {"Z": (core * 512, 512)},
        "out": {"Z": (core * 128, 128)},
        "up": {"Z": (core * 512, 128), "Q": (quarter(0), 96)},
        "down": {"Z": (core * 512, 128), "Q": (quarter(0), 96)},
    }
    sems = Sems(send, recv)
    hop1, hop2, yhop1, yin1, yhop2, yin2, d2d = {}, {}, {}, {}, {}, {}, {}
    for name in ARRAYS:
        buf = full[name]
        for part, (start, size) in parts[name].items():
            src = window(name, own[name].at[0], start, size)
            hop1[name, part, 1] = sems.remote(src, window(name, buf.at[1], start, size), up_z)
            hop1[name, part, 2] = sems.remote(src, window(name, buf.at[2], start, size), down_z)
            half = size // 2
            a, b = (start, half), (start + half, half)
            hop2[name, part, "a"] = sems.remote(window(name, buf.at[1], *a), window(name, buf.at[3], *a), up_z)
            hop2[name, part, "b"] = sems.remote(window(name, buf.at[2], *b), window(name, buf.at[3], *b), down_z)
        for slot in (1, 2, 3):
            size = depth_half[name]
            mine = window(name, buf.at[slot], core * size, size)
            d2d[name, slot] = sems.remote(mine, mine, sibling)
    for name in MLP:
        for slot in (1, 2, 3):
            buf = full[name].at[slot]

            def part(k, first_row=0, size=96, buf=buf, name=name):
                return window(name, buf, quarter(k) + first_row, size)

            for sign, to in ((1, north), (-1, south)):
                i = sems.used
                yhop1[name, slot, sign] = sems.remote(part(0), part(0), to)
                yin1[name, slot, sign] = sems.again(i, part(-sign), to)
                row = 0 if sign == 1 else 48
                i = sems.used
                yhop2[name, slot, sign] = sems.remote(part(-sign, row, 48), part(-sign, row, 48), to)
                yin2[name, slot, sign] = sems.again(i, part(2, row, 48), to)
    loads = {name: pltpu.make_async_copy(own[name].at[0], full[name].at[0], local.at[i]) for i, name in enumerate(ARRAYS)}

    def begin(name, part):
        hop1[name, part, 1].start()
        hop1[name, part, 2].start()

    def z_near(name, part):
        hop1[name, part, 1].wait_recv()
        hop2[name, part, "a"].start()
        hop1[name, part, 2].wait_recv()
        hop2[name, part, "b"].start()

    def z_far(name, part):
        hop2[name, part, "a"].wait_recv()
        hop2[name, part, "b"].wait_recv()

    def y_begin(name, *slots):
        for slot in slots:
            for sign in (1, -1):
                yhop1[name, slot, sign].start()

    def y_on(name, *slots):
        for slot in slots:
            for sign in (1, -1):
                yin1[name, slot, sign].wait_recv()
                yhop2[name, slot, sign].start()

    def y_end(name, *slots):
        for slot in slots:
            for sign in (1, -1):
                yin2[name, slot, sign].wait_recv()
            d2d[name, slot].start()

    def arrive(name, *slots):
        for slot in slots:
            d2d[name, slot].wait_recv()

    def give(name, *slots):
        for slot in slots:
            d2d[name, slot].start()

    def begin_all():
        begin("up", "Q")
        begin("down", "Q")

    def step1():
        z_near("up", "Q")
        y_begin("up", 1, 2)

    def step2():
        begin("out", "Z")
        z_near("down", "Q")
        y_begin("down", 1, 2)

    def step3():
        begin("up", "Z")
        begin("down", "Z")
        z_far("up", "Q")
        y_begin("up", 3)

    def step4():
        z_far("down", "Q")
        y_begin("down", 3)
        z_near("out", "Z")
        give("out", 1, 2)
        y_on("up", 1, 2)

    def step5():
        z_near("up", "Z")
        z_far("out", "Z")
        give("out", 3)
        arrive("out", 1, 2, 3)

    def step6():
        y_on("down", 1, 2)
        z_near("down", "Z")

    def step7():
        y_on("up", 3)
        y_end("up", 1, 2)
        y_on("down", 3)
        y_end("down", 1, 2)
        arrive("up", 1, 2)
        arrive("down", 1, 2)

    def step8():
        z_far("up", "Z")
        y_end("up", 3)
        z_far("down", "Z")
        y_end("down", 3)
        arrive("up", 3)
        arrive("down", 3)

    for name in ARRAYS:
        loads[name].start()
    gains = [pltpu.make_async_copy(gain_attn, tile.at[pl.ds(0, 1)], local.at[4]), pltpu.make_async_copy(gain_mlp, tile.at[pl.ds(8, 1)], local.at[5])]
    for g in gains:
        g.start()

    def input_copy(ref, index, k):
        return pltpu.make_async_copy(ref.at[index], h.at[k], local.at[8 + k])

    @pl.when(first == 1)
    def _():
        for k in range(4):
            seq = lax.rem(z + k, 4)

            @pl.when(seq < 2)
            def _():
                input_copy(states_q, lax.rem(seq, 2), k).start()

            @pl.when(seq >= 2)
            def _():
                input_copy(states_d, lax.rem(seq, 2), k).start()

    pl.semaphore_wait(barrier, 13)
    begin_all()
    z_low = lax.rem(z, 2)

    @pl.when(first == 0)
    def _():
        step1()
        begin("qkv", "Z")
        step2()
        step3()
        z_near("qkv", "Z")
        give("qkv", 1, 2)
        step4()
        step5()
        step6()
        z_far("qkv", "Z")
        give("qkv", 3)
        step7()
        step8()
        arrive("qkv", 1, 2, 3)

    for name in ARRAYS:
        loads[name].wait()
    for g in gains:
        g.wait()

    @pl.when(first == 1)
    def _():
        for k in range(4):
            input_copy(states_q, 0, k).wait()

    def share(k):
        return pltpu.make_async_remote_copy(
            src_ref=ctx.at[4 + k], dst_ref=ctx.at[(0, 1, 3, 2)[k]], send_sem=c_send.at[k - 1], recv_sem=c_recv.at[k - 1],
            device_id=at(z_=lax.rem(z + k, 4)), device_id_type=MESH,
        )

    nblk = S // HALF

    def hop_x(r):
        rows = pl.ds(r * HALF, HALF)
        return pltpu.make_async_remote_copy(
            src_ref=hout.at[rows], dst_ref=h.at[0, rows], send_sem=h_send.at[r], recv_sem=h_recv.at[r],
            device_id=at(pipe_=lax.rem(pipe + 1, 4)), device_id_type=MESH,
        )

    @pl.when(first == 0)
    def _():
        for r in range(nblk):
            hop_x(r).wait_recv()

    def length_of(seq):
        return jnp.where(seq == 0, qlen[0], jnp.where(seq == 1, qlen[1], jnp.where(seq == 2, dlen[0], dlen[1])))

    length = length_of(z)
    lane = lax.broadcasted_iota(jnp.int32, (1, G), 1)
    head = lane // 64
    krow = lax.broadcasted_iota(jnp.int32, (G, 1), 0)
    one, zero = jnp.ones((), BF), jnp.zeros((), BF)

    @pl.loop(0, 4)
    def _(j):
        ahead = first * lax.rem(j + 1, 4)
        group = (1 - first) * j
        bias = jnp.where(lax.broadcasted_iota(jnp.int32, (1, S), 1) < length_of(lax.rem(z + ahead, 4)), 0.0, -1e30).astype(BF)

        @pl.when((first == 1) & (j == 1))
        def _():
            share(1).start()
            step1()

        @pl.when((first == 1) & (j == 2))
        def _():
            share(2).start()
            step2()

        @pl.when((first == 1) & (j == 3))
        def _():
            share(3).start()
            step3()

        @pl.loop(0, 3)
        def _(i):
            scale = jnp.where(i == 0, 0.125 * LOG2E, jnp.where(i == 2, VSCALE, 1.0)).astype(F32)
            qkv[i] = (dot(h[ahead], b_qkv[group, i]) * scale).astype(BF)

        kt[...] = qkv[1].T
        for hd in range(4):
            nxt = (hd + 1) % 4
            mine, other, mark = head == hd, head == nxt, lane == nxt * 64
            qm[hd] = jnp.where(mine, qkv[0], jnp.where(mark, one, zero))
            km[hd] = jnp.where(krow == nxt * 64, bias, kt[...])
            vm[hd] = jnp.where(mine, qkv[2], jnp.where(other, one, zero))
        for hd in range(4):
            mine = head == hd
            for r in range(2):
                rows = slice(r * 256, (r + 1) * 256)
                p = jnp.exp2(dot(qm[hd, rows, :], km[hd])).astype(BF)
                o = dot(p, vm[hd])
                total = pltpu.roll(o, 192, 1)
                t = jnp.where(total > 2.0**60, 2.0**-64, 1.0).astype(F32)
                c = (o * t) * (1.0 / (total * t)) * (1.0 / VSCALE)
                cf[rows, :] = jnp.where(mine, c, cf[rows, :] if hd else c)
        ctx[group + ahead + 4 * ((ahead + 3) // 4)] = cf[...].astype(BF)

    @pl.when(first == 1)
    def _():
        step4()
        step5()
        for k in range(1, 4):
            share(k).wait_recv()

    @pl.loop(0, 4)
    def _(n):
        cs = pl.ds(pl.multiple_of(n * 256, 256), 256)
        acc[:, cs] = sum(dot(ctx[j], b_out[j, :, cs]) for j in range(4))

    @pl.loop(0, 4)
    def _(r):
        for q in range(4):
            rows = pl.ds(pl.multiple_of(r * 128 + q * 32, 32), 32)
            mixed[rows, :] = norm_rows(h[0, rows, :].astype(F32) + acc[rows, :], tile[0:1, :]).astype(BF)

    @pl.loop(0, 4 * nblk)
    def _(i):
        j = first * (i // nblk) + (1 - first) * lax.rem(i, 4)
        r = first * lax.rem(i, nblk) + (1 - first) * (i // 4)

        @pl.when((first == 1) & (i == 0))
        def _():
            step6()

        @pl.when((first == 1) & (i == nblk))
        def _():
            step7()

        @pl.when((first == 1) & (i == 3 * nblk))
        def _():
            step8()

        rows = pl.ds(pl.multiple_of(r * HALF, HALF), HALF)

        @pl.loop(0, 4)
        def _(n):
            cs = pl.ds(pl.multiple_of(n * 256, 256), 256)
            act[:, cs] = gelu(dot(mixed[rows, :], b_up[j, :, cs])).astype(BF)

        @pl.loop(0, 4)
        def _(n):
            cs = pl.ds(pl.multiple_of(n * 256, 256), 256)
            part = dot(act[...], b_down[j, :, cs])
            acc[rows, cs] = jnp.where(j == 0, part, acc[rows, cs] + part)

        @pl.when(j == 3)
        def _():
            @pl.loop(0, HALF // 64)
            def _(q):
                for u in range(2):
                    rr = pl.ds(pl.multiple_of(r * HALF + q * 64 + u * 32, 32), 32)
                    hout[rr, :] = norm_rows(mixed[rr, :].astype(F32) + acc[rr, :], tile[8:9, :]).astype(BF)

            for rs in range(nblk):

                @pl.when((pipe < 3) & (r == rs))
                def _():
                    hop_x(rs).start()

    def t1(k):
        return pltpu.make_async_remote_copy(
            src_ref=dtab.at[z_low, dp], dst_ref=dtab.at[z_low, dp], send_sem=t1_send.at[k - 1], recv_sem=t1_recv.at[k - 1],
            device_id=at(dp_=lax.rem(dp + k, 8)), device_id_type=MESH,
        )

    def t1_in(k):
        there = lax.rem(dp + 8 - k, 8)
        return pltpu.make_async_remote_copy(
            src_ref=dtab.at[z_low, there], dst_ref=dtab.at[z_low, there], send_sem=t1_send.at[k - 1], recv_sem=t1_recv.at[k - 1],
            device_id=at(dp_=lax.rem(dp + k, 8)), device_id_type=MESH,
        )

    def t2(tab, slot, k):
        return pltpu.make_async_remote_copy(
            src_ref=tab.at[slot], dst_ref=tab.at[slot], send_sem=t2_send.at[k - 1], recv_sem=t2_recv.at[k - 1],
            device_id=at(z_=lax.rem(z + k, 4)), device_id_type=MESH,
        )

    def t3(tab, i, k):
        return pltpu.make_async_remote_copy(
            src_ref=tab, dst_ref=tab, send_sem=t3_send.at[i, k], recv_sem=t3_recv.at[i], device_id=at(pipe_=k), device_id_type=MESH
        )

    @pl.when(pipe < 3)
    def _():
        t3(qtab, 0, 0).wait_recv()
        t3(dtab, 1, 0).wait_recv()

    @pl.when(pipe == 3)
    def _():
        acc[0:8, :] = jnp.zeros((8, D), F32)

        @pl.loop(0, 16)
        def _(r):
            rows = pl.ds(pl.multiple_of(r * 32, 32), 32)
            keep = lax.broadcasted_iota(jnp.int32, (32, 1), 0) + r * 32 < length
            x = jnp.where(keep, hout[rows, :].astype(F32), 0.0)
            acc[0:8, :] += x[0:8] + x[8:16] + x[16:24] + x[24:32]

        pooled = jnp.sum(acc[0:8, :], axis=0, keepdims=True) / length.astype(F32)
        emb = pooled * lax.rsqrt(jnp.sum(pooled * pooled, axis=-1, keepdims=True) + 1e-6)
        emb = emb.astype(BF).astype(F32)

        @pl.when(z < 2)
        def _():
            for k in range(8):
                qtab[z_low, k : k + 1, :] = emb[:, k * 128 : (k + 1) * 128]

        @pl.when(z >= 2)
        def _():
            for k in range(8):
                dtab[z_low, dp, k : k + 1, :] = emb[:, k * 128 : (k + 1) * 128]
            for k in range(1, 8):
                t1(k).start()
            for k in range(1, 8):
                t1_in(k).wait_recv()
            for k in range(1, 4):
                t2(dtab, z_low, k).start()

        @pl.when(z < 2)
        def _():
            for k in range(1, 4):
                t2(qtab, z_low, k).start()

        for k in range(1, 4):
            there = lax.rem(z + 4 - k, 4)

            @pl.when(there < 2)
            def _():
                t2(qtab, lax.rem(there, 2), k).wait_recv()

            @pl.when(there >= 2)
            def _():
                t2(dtab, lax.rem(there, 2), k).wait_recv()

        for k in range(3):
            t3(qtab, 0, k).start()
            t3(dtab, 1, k).start()

    doc_dp = lax.broadcasted_iota(jnp.int32, (8, 1), 0)
    for i in range(2):
        total, positive = jnp.zeros((1, 1), F32), jnp.zeros((1, 1), F32)
        for s in range(2):
            prod = dtab[s] * qtab[i][None]
            score = jnp.sum(jnp.sum(prod, axis=1), axis=1, keepdims=True) / 0.05
            total += jnp.sum(jnp.exp(score), axis=0, keepdims=True)
            hit = (doc_dp == dp) & (order[0, i] == s)
            positive += jnp.sum(jnp.where(hit, score, 0.0), axis=0, keepdims=True)
        out_loss[i : i + 1, :] = jnp.broadcast_to(jnp.log(total) - positive, (1, 128))
    piece = pipe * 4 + z
    row, side = piece // 2, lax.rem(piece, 2)
    for i in range(2):
        qrow = qtab[i, pl.ds(row, 1), :]
        out_q[i : i + 1, :] = jnp.where(side == 0, qrow, pltpu.roll(qrow, 64, 1))[:, :64].astype(BF)
        drow = dtab[i, dp, pl.ds(row, 1), :]
        out_d[i : i + 1, :] = jnp.where(side == 0, drow, pltpu.roll(drow, 64, 1))[:, :64].astype(BF)

    for table in (hop1, hop2, yhop1, yhop2, d2d):
        for key, copy in table.items():
            if key[0] != "qkv":
                copy.wait_send()

    @pl.when(first == 0)
    def _():
        for table in (hop1, hop2, d2d):
            for key, copy in table.items():
                if key[0] == "qkv":
                    copy.wait_send()

    @pl.when(first == 1)
    def _():
        for k in range(1, 4):
            share(k).wait_send()

    @pl.when(pipe < 3)
    def _():
        for r in range(nblk):
            hop_x(r).wait_send()

    @pl.when(pipe == 3)
    def _():
        for k in range(3):
            t3(qtab, 0, k).wait_send()
            t3(dtab, 1, k).wait_send()

        @pl.when(z >= 2)
        def _():
            for k in range(1, 8):
                t1(k).wait_send()
            for k in range(1, 4):
                t2(dtab, z_low, k).wait_send()

        @pl.when(z < 2)
        def _():
            for k in range(1, 4):
                t2(qtab, z_low, k).wait_send()


def per_device(query_states, doc_states, query_len, doc_len, doc_order, w_qkv, w_out, w_up, w_down, gain_attn, gain_mlp):
    anyspace = pl.BlockSpec(memory_space=pl.ANY)
    smem = pl.BlockSpec(memory_space=pltpu.SMEM)
    vmem = pl.BlockSpec(memory_space=pltpu.VMEM)
    q, d, loss = pl.pallas_call(
        kernel,
        out_shape=(jax.ShapeDtypeStruct((2, 64), BF), jax.ShapeDtypeStruct((2, 64), BF), jax.ShapeDtypeStruct((2, 128), F32)),
        in_specs=[anyspace, anyspace, smem, smem, smem, *[anyspace] * 6],
        out_specs=(vmem, vmem, vmem),
        scratch_shapes=[
            pltpu.VMEM((4, 3, D, G), BF),
            pltpu.VMEM((4, G, D), BF),
            pltpu.VMEM((4, D, D), BF),
            pltpu.VMEM((4, D, D), BF),
            pltpu.VMEM((4, S, D), BF),
            pltpu.VMEM((S, D), BF),
            pltpu.VMEM((3, S, G), BF),
            pltpu.VMEM((4, S, G), BF),
            pltpu.VMEM((4, G, S), BF),
            pltpu.VMEM((G, S), BF),
            pltpu.VMEM((4, S, G), BF),
            pltpu.VMEM((S, G), F32),
            pltpu.VMEM((8, S, G), BF),
            pltpu.VMEM((S, D), F32),
            pltpu.VMEM((S, D), BF),
            pltpu.VMEM((HALF, D), BF),
            pltpu.VMEM((2, 8, 128), F32),
            pltpu.VMEM((2, 8, 8, 128), F32),
            pltpu.VMEM((16, D), F32),
            pltpu.SemaphoreType.DMA((N_SEMS,)),
            pltpu.SemaphoreType.DMA((N_SEMS,)),
            pltpu.SemaphoreType.DMA((12,)),
            pltpu.SemaphoreType.DMA((3,)),
            pltpu.SemaphoreType.DMA((3,)),
            pltpu.SemaphoreType.DMA((S // HALF,)),
            pltpu.SemaphoreType.DMA((S // HALF,)),
            pltpu.SemaphoreType.DMA((7,)),
            pltpu.SemaphoreType.DMA((7,)),
            pltpu.SemaphoreType.DMA((3,)),
            pltpu.SemaphoreType.DMA((3,)),
            pltpu.SemaphoreType.DMA((2, 3)),
            pltpu.SemaphoreType.DMA((2,)),
        ],
        compiler_params=pltpu.CompilerParams(collective_id=0, has_side_effects=True, vmem_limit_bytes=63 * 2**20),
        name="encode",
    )(query_states, doc_states, query_len, doc_len, doc_order, w_qkv, w_out, w_up, w_down, gain_attn, gain_mlp)
    return q, d, loss[:, 0]


def solution(mesh):
    in_specs = (
        P("dp", None, None),
        P("dp", None, None),
        P("dp"),
        P("dp"),
        P("dp", None),
        P("pipe", None, None, "tensor"),
        P("pipe", "tensor", None),
        P("pipe", None, "tensor"),
        P("pipe", "tensor", None),
        P("pipe", None),
        P("pipe", None),
    )
    out_specs = (P("dp", ("pipe", "tensor")), P("dp", ("pipe", "tensor")), P("dp"))
    return jax.shard_map(per_device, mesh=mesh, in_specs=in_specs, out_specs=out_specs, check_vma=False)
```

```python
import jax
import jax.numpy as jnp
from jax import lax
from jax.experimental import pallas as pl
from jax.experimental.pallas import tpu as pltpu
from jax.sharding import PartitionSpec as P

S = 512
D = 1024
G = 256
HALF = 256
BF = jnp.bfloat16
F32 = jnp.float32
LOG2E = 1.4426950408889634
VSCALE = 2.0**-14
SQRT_HALF = 0.7071067811865476
MESH = pl.DeviceIdType.MESH
ARRAYS = ("qkv", "out", "up", "down")
MLP = ("up", "down")
depth_half = {"qkv": 512, "out": 128, "up": 512, "down": 512}


def dot(a, b):
    return jnp.dot(a, b, preferred_element_type=F32)


def norm_rows(x, gain):
    mean = jnp.mean(x, axis=-1, keepdims=True)
    centered = x - mean
    variance = jnp.mean(centered * centered, axis=-1, keepdims=True)
    return centered * lax.rsqrt(variance + 1e-12) * gain


def gelu(u):
    return 0.5 * u * (1.0 + lax.erf(u * SQRT_HALF))


class Sems:
    def __init__(self, send, recv):
        self.send, self.recv, self.used = send, recv, 0

    def remote(self, src, dst, device):
        i = self.used
        self.used += 1
        return pltpu.make_async_remote_copy(
            src_ref=src, dst_ref=dst, send_sem=self.send.at[i], recv_sem=self.recv.at[i], device_id=device, device_id_type=MESH
        )


    def again(self, i, ref, device):
        return pltpu.make_async_remote_copy(
            src_ref=ref, dst_ref=ref, send_sem=self.send.at[i], recv_sem=self.recv.at[i], device_id=device, device_id_type=MESH
        )


N_SEMS = 60


def kernel(
    states_q, states_d, qlen, dlen, order, w_qkv, w_out, w_up, w_down, gain_attn, gain_mlp,
    out,
    b_qkv, b_out, b_up, b_down, h, hout, qkv, qm, km, kt, vm, cf, ctx, acc, mixed, act, qtab, dtab, pieces, tile,
    send, recv, local, c_send, c_recv, h_send, h_recv, t1_send, t1_recv, t2_send, t2_recv, t3_send, t3_recv,
):
    dp, pipe, z = lax.axis_index("dp"), lax.axis_index("pipe"), lax.axis_index("tensor")
    core = lax.rem(dp, 2)
    first = 1 - (pipe + 3) // 4

    def at(dp_=dp, pipe_=pipe, z_=z):
        return (dp_, pipe_, z_)

    up_z, down_z = at(z_=lax.rem(z + 1, 4)), at(z_=lax.rem(z + 3, 4))
    sibling = at(dp_=dp + 1 - 2 * core)

    barrier = pltpu.get_barrier_semaphore()
    for k in range(1, 8):
        pl.semaphore_signal(barrier, inc=1, device_id=at(dp_=lax.rem(dp + k, 8)), device_id_type=MESH)
    for k in range(1, 4):
        pl.semaphore_signal(barrier, inc=1, device_id=at(pipe_=lax.rem(pipe + k, 4)), device_id_type=MESH)
        pl.semaphore_signal(barrier, inc=1, device_id=at(z_=lax.rem(z + k, 4)), device_id_type=MESH)

    y = dp // 2
    own = {"qkv": w_qkv, "out": w_out, "up": w_up, "down": w_down}
    full = {"qkv": b_qkv, "out": b_out, "up": b_up, "down": b_down}
    north, south = at(dp_=lax.rem(dp + 2, 8)), at(dp_=lax.rem(dp + 6, 8))

    def window(name, ref, start, size):
        sl = pl.ds(pl.multiple_of(start, 16), size)
        return ref.at[:, sl, :] if name == "qkv" else ref.at[sl, :]

    def quarter(k):
        return core * 512 + 128 + 96 * lax.rem(y + k + 4, 4)

    parts = {
        "qkv": {"Z": (core * 512, 512)},
        "out": {"Z": (core * 128, 128)},
        "up": {"Z": (core * 512, 128), "Q": (quarter(0), 96)},
        "down": {"Z": (core * 512, 128), "Q": (quarter(0), 96)},
    }
    sems = Sems(send, recv)
    hop1, hop2, yhop1, yin1, yhop2, yin2, d2d = {}, {}, {}, {}, {}, {}, {}
    for name in ARRAYS:
        buf = full[name]
        for part, (start, size) in parts[name].items():
            src = window(name, own[name].at[0], start, size)
            hop1[name, part, 1] = sems.remote(src, window(name, buf.at[1], start, size), up_z)
            hop1[name, part, 2] = sems.remote(src, window(name, buf.at[2], start, size), down_z)
            half = size // 2
            a, b = (start, half), (start + half, half)
            hop2[name, part, "a"] = sems.remote(window(name, buf.at[1], *a), window(name, buf.at[3], *a), up_z)
            hop2[name, part, "b"] = sems.remote(window(name, buf.at[2], *b), window(name, buf.at[3], *b), down_z)
        for slot in (1, 2, 3):
            size = depth_half[name]
            mine = window(name, buf.at[slot], core * size, size)
            d2d[name, slot] = sems.remote(mine, mine, sibling)
    for name in MLP:
        for slot in (1, 2, 3):
            buf = full[name].at[slot]

            def part(k, first_row=0, size=96, buf=buf, name=name):
                return window(name, buf, quarter(k) + first_row, size)

            for sign, to in ((1, north), (-1, south)):
                i = sems.used
                yhop1[name, slot, sign] = sems.remote(part(0), part(0), to)
                yin1[name, slot, sign] = sems.again(i, part(-sign), to)
                row = 0 if sign == 1 else 48
                i = sems.used
                yhop2[name, slot, sign] = sems.remote(part(-sign, row, 48), part(-sign, row, 48), to)
                yin2[name, slot, sign] = sems.again(i, part(2, row, 48), to)
    loads = {name: pltpu.make_async_copy(own[name].at[0], full[name].at[0], local.at[i]) for i, name in enumerate(ARRAYS)}

    def begin(name, part):
        hop1[name, part, 1].start()
        hop1[name, part, 2].start()

    def z_near(name, part):
        hop1[name, part, 1].wait_recv()
        hop2[name, part, "a"].start()
        hop1[name, part, 2].wait_recv()
        hop2[name, part, "b"].start()

    def z_far(name, part):
        hop2[name, part, "a"].wait_recv()
        hop2[name, part, "b"].wait_recv()

    def y_begin(name, *slots):
        for slot in slots:
            for sign in (1, -1):
                yhop1[name, slot, sign].start()

    def y_on(name, *slots):
        for slot in slots:
            for sign in (1, -1):
                yin1[name, slot, sign].wait_recv()
                yhop2[name, slot, sign].start()

    def y_end(name, *slots):
        for slot in slots:
            for sign in (1, -1):
                yin2[name, slot, sign].wait_recv()
            d2d[name, slot].start()

    def arrive(name, *slots):
        for slot in slots:
            d2d[name, slot].wait_recv()

    def give(name, *slots):
        for slot in slots:
            d2d[name, slot].start()

    def begin_all():
        begin("up", "Q")
        begin("down", "Q")

    def step1():
        z_near("up", "Q")
        y_begin("up", 1, 2)

    def step2():
        begin("out", "Z")
        z_near("down", "Q")
        y_begin("down", 1, 2)

    def step3():
        begin("up", "Z")
        begin("down", "Z")
        z_far("up", "Q")
        y_begin("up", 3)

    def step4():
        z_far("down", "Q")
        y_begin("down", 3)
        z_near("out", "Z")
        give("out", 1, 2)
        y_on("up", 1, 2)

    def step5():
        z_near("up", "Z")
        z_far("out", "Z")
        give("out", 3)
        arrive("out", 1, 2, 3)

    def step6():
        y_on("down", 1, 2)
        z_near("down", "Z")

    def step7():
        y_on("up", 3)
        y_end("up", 1, 2)
        y_on("down", 3)
        y_end("down", 1, 2)
        arrive("up", 1, 2)
        arrive("down", 1, 2)

    def step8():
        z_far("up", "Z")
        y_end("up", 3)
        z_far("down", "Z")
        y_end("down", 3)
        arrive("up", 3)
        arrive("down", 3)

    for name in ARRAYS:
        loads[name].start()
    gains = [pltpu.make_async_copy(gain_attn, tile.at[pl.ds(0, 1)], local.at[4]), pltpu.make_async_copy(gain_mlp, tile.at[pl.ds(8, 1)], local.at[5])]
    for g in gains:
        g.start()

    def input_copy(ref, index, k):
        return pltpu.make_async_copy(ref.at[index], h.at[k], local.at[8 + k])

    @pl.when(first == 1)
    def _():
        for k in range(4):
            seq = lax.rem(z + k, 4)

            @pl.when(seq < 2)
            def _():
                input_copy(states_q, lax.rem(seq, 2), k).start()

            @pl.when(seq >= 2)
            def _():
                input_copy(states_d, lax.rem(seq, 2), k).start()

    pl.semaphore_wait(barrier, 13)
    begin_all()
    z_low = lax.rem(z, 2)

    @pl.when(first == 0)
    def _():
        step1()
        begin("qkv", "Z")
        step2()
        step3()
        z_near("qkv", "Z")
        give("qkv", 1, 2)
        step4()
        step5()
        step6()
        z_far("qkv", "Z")
        give("qkv", 3)
        step7()
        step8()
        arrive("qkv", 1, 2, 3)

    for name in ARRAYS:
        loads[name].wait()
    for g in gains:
        g.wait()

    @pl.when(first == 1)
    def _():
        for k in range(4):
            input_copy(states_q, 0, k).wait()

    def share(k):
        return pltpu.make_async_remote_copy(
            src_ref=ctx.at[4 + k], dst_ref=ctx.at[(0, 1, 3, 2)[k]], send_sem=c_send.at[k - 1], recv_sem=c_recv.at[k - 1],
            device_id=at(z_=lax.rem(z + k, 4)), device_id_type=MESH,
        )

    nblk = S // HALF

    def hop_x(r):
        rows = pl.ds(r * HALF, HALF)
        return pltpu.make_async_remote_copy(
            src_ref=hout.at[rows], dst_ref=h.at[0, rows], send_sem=h_send.at[r], recv_sem=h_recv.at[r],
            device_id=at(pipe_=lax.rem(pipe + 1, 4)), device_id_type=MESH,
        )

    def length_of(seq):
        return jnp.where(seq == 0, qlen[0], jnp.where(seq == 1, qlen[1], jnp.where(seq == 2, dlen[0], dlen[1])))

    length = length_of(z)
    lane = lax.broadcasted_iota(jnp.int32, (1, G), 1)
    head = lane // 64
    krow = lax.broadcasted_iota(jnp.int32, (G, 1), 0)
    one, zero = jnp.ones((), BF), jnp.zeros((), BF)

    @pl.loop(0, 4)
    def _(k):
        for r in range(nblk):

            @pl.when((first == 0) & (k == 2 * r))
            def _():
                hop_x(r).wait_recv()

        for v in range(2):
            u = 2 * k + v
            ahead = first * lax.rem(u // 2 + 1, 4)
            group = (1 - first) * lax.rem(u, 4)
            block = first * v + (1 - first) * (u // 4)
            rows = pl.ds(pl.multiple_of(block * 256, 256), 256)
            for i in range(3):
                scale = (0.125 * LOG2E, 1.0, VSCALE)[i]
                qkv[ahead + group, i, rows, :] = (dot(h[ahead, rows, :], b_qkv[group, i]) * scale).astype(BF)

    @pl.when(first == 1)
    def _():
        step1()

    @pl.loop(0, 4)
    def _(j):
        ahead = first * lax.rem(j + 1, 4)
        group = (1 - first) * j
        at_ = ahead + group
        bias = jnp.where(lax.broadcasted_iota(jnp.int32, (1, S), 1) < length_of(lax.rem(z + ahead, 4)), 0.0, -1e30).astype(BF)

        for k in range(1, 4):

            @pl.when((first == 1) & (j == k))
            def _():
                share(k).start()
                if k == 2:
                    step2()

        kt[...] = qkv[at_, 1].T
        for hd in range(4):
            nxt = (hd + 1) % 4
            mine, other, mark = head == hd, head == nxt, lane == nxt * 64
            qm[hd] = jnp.where(mine, qkv[at_, 0], jnp.where(mark, one, zero))
            km[hd] = jnp.where(krow == nxt * 64, bias, kt[...])
            vm[hd] = jnp.where(mine, qkv[at_, 2], jnp.where(other, one, zero))
        for hd in range(4):
            mine = head == hd
            for r in range(2):
                rows = slice(r * 256, (r + 1) * 256)
                p = jnp.exp2(dot(qm[hd, rows, :], km[hd])).astype(BF)
                o = dot(p, vm[hd])
                total = pltpu.roll(o, 192, 1)
                t = jnp.where(total > 2.0**60, 2.0**-64, 1.0).astype(F32)
                c = (o * t) * (1.0 / (total * t)) * (1.0 / VSCALE)
                cf[rows, :] = jnp.where(mine, c, cf[rows, :] if hd else c)
        ctx[group + ahead + 4 * ((ahead + 3) // 4)] = cf[...].astype(BF)

    @pl.when(first == 1)
    def _():
        step3()
        step4()
        step5()
        for k in range(1, 4):
            share(k).wait_recv()

    for n in range(4):
        cs = slice(n * 256, (n + 1) * 256)
        acc[:, cs] = sum(dot(ctx[j], b_out[j, :, cs]) for j in range(4))

    @pl.loop(0, 4)
    def _(r):
        for q in range(4):
            rows = pl.ds(pl.multiple_of(r * 128 + q * 32, 32), 32)
            mixed[rows, :] = norm_rows(h[0, rows, :].astype(F32) + acc[rows, :], tile[0:1, :]).astype(BF)

    @pl.loop(0, 4 * nblk)
    def _(i):
        j = first * (i // nblk) + (1 - first) * lax.rem(i, 4)
        r = first * lax.rem(i, nblk) + (1 - first) * (i // 4)

        @pl.when((first == 1) & (i == 0))
        def _():
            step6()

        @pl.when((first == 1) & (i == nblk))
        def _():
            step7()

        @pl.when((first == 1) & (i == 3 * nblk))
        def _():
            step8()

        rows = pl.ds(pl.multiple_of(r * HALF, HALF), HALF)

        for n in range(4):
            cs = slice(n * 256, (n + 1) * 256)
            act[:, cs] = gelu(dot(mixed[rows, :], b_up[j, :, cs])).astype(BF)

        for n in range(4):
            cs = slice(n * 256, (n + 1) * 256)
            part = dot(act[...], b_down[j, :, cs])
            acc[rows, cs] = jnp.where(j == 0, part, acc[rows, cs] + part)

        @pl.when(j == 3)
        def _():
            @pl.loop(0, HALF // 64)
            def _(q):
                for u in range(2):
                    rr = pl.ds(pl.multiple_of(r * HALF + q * 64 + u * 32, 32), 32)
                    hout[rr, :] = norm_rows(mixed[rr, :].astype(F32) + acc[rr, :], tile[8:9, :]).astype(BF)

            for rs in range(nblk):

                @pl.when((pipe < 3) & (r == rs))
                def _():
                    hop_x(rs).start()

    def t1(k):
        return pltpu.make_async_remote_copy(
            src_ref=dtab.at[z_low, dp], dst_ref=dtab.at[z_low, dp], send_sem=t1_send.at[k - 1], recv_sem=t1_recv.at[k - 1],
            device_id=at(dp_=lax.rem(dp + k, 8)), device_id_type=MESH,
        )

    def t1_in(k):
        there = lax.rem(dp + 8 - k, 8)
        return pltpu.make_async_remote_copy(
            src_ref=dtab.at[z_low, there], dst_ref=dtab.at[z_low, there], send_sem=t1_send.at[k - 1], recv_sem=t1_recv.at[k - 1],
            device_id=at(dp_=lax.rem(dp + k, 8)), device_id_type=MESH,
        )

    def t2(tab, slot, k):
        return pltpu.make_async_remote_copy(
            src_ref=tab.at[slot], dst_ref=tab.at[slot], send_sem=t2_send.at[k - 1], recv_sem=t2_recv.at[k - 1],
            device_id=at(z_=lax.rem(z + k, 4)), device_id_type=MESH,
        )

    def t3(k):
        return pltpu.make_async_remote_copy(
            src_ref=pieces.at[k], dst_ref=pieces.at[4], send_sem=t3_send.at[k], recv_sem=t3_recv.at[0], device_id=at(pipe_=k), device_id_type=MESH
        )

    @pl.when(pipe < 3)
    def _():
        t3(0).wait_recv()

    @pl.when(pipe == 3)
    def _():
        acc[0:8, :] = jnp.zeros((8, D), F32)

        @pl.loop(0, 16)
        def _(r):
            rows = pl.ds(pl.multiple_of(r * 32, 32), 32)
            keep = lax.broadcasted_iota(jnp.int32, (32, 1), 0) + r * 32 < length
            x = jnp.where(keep, hout[rows, :].astype(F32), 0.0)
            acc[0:8, :] += x[0:8] + x[8:16] + x[16:24] + x[24:32]

        pooled = jnp.sum(acc[0:8, :], axis=0, keepdims=True) / length.astype(F32)
        emb = pooled * lax.rsqrt(jnp.sum(pooled * pooled, axis=-1, keepdims=True) + 1e-6)
        emb = emb.astype(BF).astype(F32)

        @pl.when(z < 2)
        def _():
            for k in range(8):
                qtab[z_low, k : k + 1, :] = emb[:, k * 128 : (k + 1) * 128]

        @pl.when(z >= 2)
        def _():
            for k in range(8):
                dtab[z_low, dp, k : k + 1, :] = emb[:, k * 128 : (k + 1) * 128]
            for k in range(1, 8):
                t1(k).start()
            for k in range(1, 8):
                t1_in(k).wait_recv()
            for k in range(1, 4):
                t2(dtab, z_low, k).start()

        @pl.when(z < 2)
        def _():
            for k in range(1, 4):
                t2(qtab, z_low, k).start()

        for k in range(1, 4):
            there = lax.rem(z + 4 - k, 4)

            @pl.when(there < 2)
            def _():
                t2(qtab, lax.rem(there, 2), k).wait_recv()

            @pl.when(there >= 2)
            def _():
                t2(dtab, lax.rem(there, 2), k).wait_recv()

        doc_dp = lax.broadcasted_iota(jnp.int32, (8, 1), 0)
        losses = []
        for i in range(2):
            total, positive = jnp.zeros((1, 1), F32), jnp.zeros((1, 1), F32)
            for s in range(2):
                prod = dtab[s] * qtab[i][None]
                score = jnp.sum(jnp.sum(prod, axis=1), axis=1, keepdims=True) / 0.05
                total += jnp.sum(jnp.exp(score), axis=0, keepdims=True)
                hit = (doc_dp == dp) & (order[0, i] == s)
                positive += jnp.sum(jnp.where(hit, score, 0.0), axis=0, keepdims=True)
            losses.append(jnp.broadcast_to(jnp.log(total) - positive, (1, 128)))
        for k in (0, 1, 2, 3):
            row = 2 * k + z // 2
            pieces[k, 6:8, :] = jnp.zeros((2, 128), F32)
            for i in range(2):
                for at_row, line in ((i, qtab[i, pl.ds(row, 1), :]), (2 + i, dtab[i, dp, pl.ds(row, 1), :])):
                    pieces[k, at_row : at_row + 1, :] = jnp.where(z_low == 0, line, pltpu.roll(line, 64, 1))
                pieces[k, 4 + i : 5 + i, :] = losses[i]
            if k < 3:
                t3(k).start()
        pieces[4] = pieces[3]

    out[...] = pieces[4]

    for table in (hop1, hop2, yhop1, yhop2, d2d):
        for key, copy in table.items():
            if key[0] != "qkv":
                copy.wait_send()

    @pl.when(first == 0)
    def _():
        for table in (hop1, hop2, d2d):
            for key, copy in table.items():
                if key[0] == "qkv":
                    copy.wait_send()

    @pl.when(first == 1)
    def _():
        for k in range(1, 4):
            share(k).wait_send()

    @pl.when(pipe < 3)
    def _():
        for r in range(nblk):
            hop_x(r).wait_send()

    @pl.when(pipe == 3)
    def _():
        for k in range(3):
            t3(k).wait_send()

        @pl.when(z >= 2)
        def _():
            for k in range(1, 8):
                t1(k).wait_send()
            for k in range(1, 4):
                t2(dtab, z_low, k).wait_send()

        @pl.when(z < 2)
        def _():
            for k in range(1, 4):
                t2(qtab, z_low, k).wait_send()


def per_device(query_states, doc_states, query_len, doc_len, doc_order, w_qkv, w_out, w_up, w_down, gain_attn, gain_mlp):
    anyspace = pl.BlockSpec(memory_space=pl.ANY)
    smem = pl.BlockSpec(memory_space=pltpu.SMEM)
    vmem = pl.BlockSpec(memory_space=pltpu.VMEM)
    out = pl.pallas_call(
        kernel,
        out_shape=jax.ShapeDtypeStruct((8, 128), F32),
        in_specs=[anyspace, anyspace, smem, smem, smem, *[anyspace] * 6],
        out_specs=vmem,
        scratch_shapes=[
            pltpu.VMEM((4, 3, D, G), BF),
            pltpu.VMEM((4, G, D), BF),
            pltpu.VMEM((4, D, D), BF),
            pltpu.VMEM((4, D, D), BF),
            pltpu.VMEM((4, S, D), BF),
            pltpu.VMEM((S, D), BF),
            pltpu.VMEM((4, 3, S, G), BF),
            pltpu.VMEM((4, S, G), BF),
            pltpu.VMEM((4, G, S), BF),
            pltpu.VMEM((G, S), BF),
            pltpu.VMEM((4, S, G), BF),
            pltpu.VMEM((S, G), F32),
            pltpu.VMEM((8, S, G), BF),
            pltpu.VMEM((S, D), F32),
            pltpu.VMEM((S, D), BF),
            pltpu.VMEM((HALF, D), BF),
            pltpu.VMEM((2, 8, 128), F32),
            pltpu.VMEM((2, 8, 8, 128), F32),
            pltpu.VMEM((5, 8, 128), F32),
            pltpu.VMEM((16, D), F32),
            pltpu.SemaphoreType.DMA((N_SEMS,)),
            pltpu.SemaphoreType.DMA((N_SEMS,)),
            pltpu.SemaphoreType.DMA((12,)),
            pltpu.SemaphoreType.DMA((3,)),
            pltpu.SemaphoreType.DMA((3,)),
            pltpu.SemaphoreType.DMA((S // HALF,)),
            pltpu.SemaphoreType.DMA((S // HALF,)),
            pltpu.SemaphoreType.DMA((7,)),
            pltpu.SemaphoreType.DMA((7,)),
            pltpu.SemaphoreType.DMA((3,)),
            pltpu.SemaphoreType.DMA((3,)),
            pltpu.SemaphoreType.DMA((3,)),
            pltpu.SemaphoreType.DMA((1,)),
        ],
        compiler_params=pltpu.CompilerParams(collective_id=0, has_side_effects=True, vmem_limit_bytes=63 * 2**20),
        name="encode",
    )(query_states, doc_states, query_len, doc_len, doc_order, w_qkv, w_out, w_up, w_down, gain_attn, gain_mlp)
    return out[0:2, :64].astype(BF), out[2:4, :64].astype(BF), out[4:6, 0]


def solution(mesh):
    in_specs = (
        P("dp", None, None),
        P("dp", None, None),
        P("dp"),
        P("dp"),
        P("dp", None),
        P("pipe", None, None, "tensor"),
        P("pipe", "tensor", None),
        P("pipe", None, "tensor"),
        P("pipe", "tensor", None),
        P("pipe", None),
        P("pipe", None),
    )
    out_specs = (P("dp", ("pipe", "tensor")), P("dp", ("pipe", "tensor")), P("dp"))
    return jax.shard_map(per_device, mesh=mesh, in_specs=in_specs, out_specs=out_specs, check_vma=False)
```

```python
import jax
import jax.numpy as jnp
from jax import lax
from jax.experimental import pallas as pl
from jax.experimental.pallas import tpu as pltpu
from jax.sharding import PartitionSpec as P

S = 512
D = 1024
G = 256
HALF = 256
BF = jnp.bfloat16
F32 = jnp.float32
LOG2E = 1.4426950408889634
VSCALE = 2.0**-14
SQRT_HALF = 0.7071067811865476
MESH = pl.DeviceIdType.MESH
ARRAYS = ("qkv", "out", "up", "down")
MLP = ("up", "down")
depth_half = {"qkv": 512, "out": 128, "up": 512, "down": 512}


def dot(a, b):
    return jnp.dot(a, b, preferred_element_type=F32)


def norm_rows(x, gain):
    mean = jnp.mean(x, axis=-1, keepdims=True)
    centered = x - mean
    variance = jnp.mean(centered * centered, axis=-1, keepdims=True)
    return centered * lax.rsqrt(variance + 1e-12) * gain


def gelu(u):
    return 0.5 * u * (1.0 + lax.erf(u * SQRT_HALF))


class Sems:
    def __init__(self, send, recv):
        self.send, self.recv, self.used = send, recv, 0

    def remote(self, src, dst, device):
        i = self.used
        self.used += 1
        return pltpu.make_async_remote_copy(
            src_ref=src, dst_ref=dst, send_sem=self.send.at[i], recv_sem=self.recv.at[i], device_id=device, device_id_type=MESH
        )


    def again(self, i, ref, device):
        return pltpu.make_async_remote_copy(
            src_ref=ref, dst_ref=ref, send_sem=self.send.at[i], recv_sem=self.recv.at[i], device_id=device, device_id_type=MESH
        )


N_SEMS = 60


def kernel(
    states_q, states_d, qlen, dlen, order, w_qkv, w_out, w_up, w_down, gain_attn, gain_mlp,
    out,
    b_qkv, b_out, b_up, b_down, h, hout, qkv, qm, km, kt, vm, cf, ctx, relay, acc, mixed, act, qtab, dtab, pieces, tile,
    send, recv, local, c_send, c_recv, h_send, h_recv, t1_send, t1_recv, t2_send, t2_recv, t3_send, t3_recv,
):
    dp, pipe, z = lax.axis_index("dp"), lax.axis_index("pipe"), lax.axis_index("tensor")
    core = lax.rem(dp, 2)
    first = 1 - (pipe + 3) // 4

    def at(dp_=dp, pipe_=pipe, z_=z):
        return (dp_, pipe_, z_)

    up_z, down_z = at(z_=lax.rem(z + 1, 4)), at(z_=lax.rem(z + 3, 4))
    sibling = at(dp_=dp + 1 - 2 * core)

    barrier = pltpu.get_barrier_semaphore()
    for k in range(1, 8):
        pl.semaphore_signal(barrier, inc=1, device_id=at(dp_=lax.rem(dp + k, 8)), device_id_type=MESH)
    for k in range(1, 4):
        pl.semaphore_signal(barrier, inc=1, device_id=at(pipe_=lax.rem(pipe + k, 4)), device_id_type=MESH)
        pl.semaphore_signal(barrier, inc=1, device_id=at(z_=lax.rem(z + k, 4)), device_id_type=MESH)

    y = dp // 2
    own = {"qkv": w_qkv, "out": w_out, "up": w_up, "down": w_down}
    full = {"qkv": b_qkv, "out": b_out, "up": b_up, "down": b_down}
    north, south = at(dp_=lax.rem(dp + 2, 8)), at(dp_=lax.rem(dp + 6, 8))

    def window(name, ref, start, size):
        sl = pl.ds(pl.multiple_of(start, 16), size)
        return ref.at[:, sl, :] if name == "qkv" else ref.at[sl, :]

    def quarter(k):
        return core * 512 + 128 + 96 * lax.rem(y + k + 4, 4)

    parts = {
        "qkv": {"Z": (core * 512, 512)},
        "out": {"Z": (core * 128, 128)},
        "up": {"Z": (core * 512, 128), "Q": (quarter(0), 96)},
        "down": {"Z": (core * 512, 128), "Q": (quarter(0), 96)},
    }
    sems = Sems(send, recv)
    hop1, hop2, yhop1, yin1, yhop2, yin2, d2d = {}, {}, {}, {}, {}, {}, {}
    for name in ARRAYS:
        buf = full[name]
        for part, (start, size) in parts[name].items():
            src = window(name, own[name].at[0], start, size)
            hop1[name, part, 1] = sems.remote(src, window(name, buf.at[1], start, size), up_z)
            hop1[name, part, 2] = sems.remote(src, window(name, buf.at[2], start, size), down_z)
            half = size // 2
            a, b = (start, half), (start + half, half)
            hop2[name, part, "a"] = sems.remote(window(name, buf.at[1], *a), window(name, buf.at[3], *a), up_z)
            hop2[name, part, "b"] = sems.remote(window(name, buf.at[2], *b), window(name, buf.at[3], *b), down_z)
        for slot in (1, 2, 3):
            size = depth_half[name]
            mine = window(name, buf.at[slot], core * size, size)
            d2d[name, slot] = sems.remote(mine, mine, sibling)
    for name in MLP:
        for slot in (1, 2, 3):
            buf = full[name].at[slot]

            def part(k, first_row=0, size=96, buf=buf, name=name):
                return window(name, buf, quarter(k) + first_row, size)

            for sign, to in ((1, north), (-1, south)):
                i = sems.used
                yhop1[name, slot, sign] = sems.remote(part(0), part(0), to)
                yin1[name, slot, sign] = sems.again(i, part(-sign), to)
                row = 0 if sign == 1 else 48
                i = sems.used
                yhop2[name, slot, sign] = sems.remote(part(-sign, row, 48), part(-sign, row, 48), to)
                yin2[name, slot, sign] = sems.again(i, part(2, row, 48), to)
    loads = {name: pltpu.make_async_copy(own[name].at[0], full[name].at[0], local.at[i]) for i, name in enumerate(ARRAYS)}

    def begin(name, part):
        hop1[name, part, 1].start()
        hop1[name, part, 2].start()

    def z_near(name, part):
        hop1[name, part, 1].wait_recv()
        hop2[name, part, "a"].start()
        hop1[name, part, 2].wait_recv()
        hop2[name, part, "b"].start()

    def z_far(name, part):
        hop2[name, part, "a"].wait_recv()
        hop2[name, part, "b"].wait_recv()

    def y_begin(name, *slots):
        for slot in slots:
            for sign in (1, -1):
                yhop1[name, slot, sign].start()

    def y_on(name, *slots):
        for slot in slots:
            for sign in (1, -1):
                yin1[name, slot, sign].wait_recv()
                yhop2[name, slot, sign].start()

    def y_end(name, *slots):
        for slot in slots:
            for sign in (1, -1):
                yin2[name, slot, sign].wait_recv()
            d2d[name, slot].start()

    def arrive(name, *slots):
        for slot in slots:
            d2d[name, slot].wait_recv()

    def give(name, *slots):
        for slot in slots:
            d2d[name, slot].start()

    def begin_all():
        begin("out", "Z")
        begin("up", "Q")
        begin("down", "Q")

    def step1():
        z_near("out", "Z")
        give("out", 1, 2)

    def step2():
        z_near("up", "Q")
        y_begin("up", 1, 2)

    def step3():
        z_near("down", "Q")
        y_begin("down", 1, 2)

    def step4():
        z_far("out", "Z")
        give("out", 3)
        z_far("up", "Q")
        y_begin("up", 3)
        y_on("up", 1, 2)

    def step5():
        begin("up", "Z")
        begin("down", "Z")
        y_on("down", 1, 2)
        z_far("down", "Q")
        y_begin("down", 3)
        arrive("out", 1, 2, 3)

    def step6():
        y_on("up", 3)

    def step7():
        z_near("up", "Z")
        y_end("up", 1, 2)
        y_on("down", 3)
        z_near("down", "Z")
        y_end("down", 1, 2)
        arrive("up", 1, 2)
        arrive("down", 1, 2)

    def step8():
        z_far("up", "Z")
        y_end("up", 3)
        z_far("down", "Z")
        y_end("down", 3)
        arrive("up", 3)
        arrive("down", 3)

    for name in ARRAYS:
        loads[name].start()
    gains = [pltpu.make_async_copy(gain_attn, tile.at[pl.ds(0, 1)], local.at[4]), pltpu.make_async_copy(gain_mlp, tile.at[pl.ds(8, 1)], local.at[5])]
    for g in gains:
        g.start()

    def input_copy(ref, index, k):
        return pltpu.make_async_copy(ref.at[index], h.at[k], local.at[8 + k])

    @pl.when(first == 1)
    def _():
        for k in range(4):
            seq = lax.rem(z + k, 4)

            @pl.when(seq < 2)
            def _():
                input_copy(states_q, lax.rem(seq, 2), k).start()

            @pl.when(seq >= 2)
            def _():
                input_copy(states_d, lax.rem(seq, 2), k).start()

    pl.semaphore_wait(barrier, 13)
    begin_all()
    z_low = lax.rem(z, 2)

    @pl.when(first == 0)
    def _():
        step1()
        step2()
        begin("qkv", "Z")
        step3()
        step4()
        step5()
        z_near("qkv", "Z")
        give("qkv", 1, 2)
        step6()
        step7()
        z_far("qkv", "Z")
        give("qkv", 3)
        step8()
        arrive("qkv", 1, 2, 3)

    for name in ARRAYS:
        loads[name].wait()
    for g in gains:
        g.wait()

    @pl.when(first == 1)
    def _():
        for k in range(4):
            input_copy(states_q, 0, k).wait()

    def to_z(i, src, dst, k):
        return pltpu.make_async_remote_copy(
            src_ref=src, dst_ref=dst, send_sem=c_send.at[i], recv_sem=c_recv.at[i], device_id=at(z_=lax.rem(z + k, 4)), device_id_type=MESH
        )

    top, bottom = pl.ds(0, 256), pl.ds(256, 256)
    share = {
        1: (to_z(0, ctx.at[5], ctx.at[1], 1),),
        3: (to_z(1, ctx.at[7], ctx.at[2], 3),),
        2: (to_z(2, ctx.at[6, top], relay.at[0], 1), to_z(3, ctx.at[6, bottom], relay.at[1], 3)),
    }
    share_on = (to_z(4, relay.at[0], ctx.at[3, top], 1), to_z(5, relay.at[1], ctx.at[3, bottom], 3))

    nblk = S // HALF

    def hop_x(r):
        rows = pl.ds(r * HALF, HALF)
        return pltpu.make_async_remote_copy(
            src_ref=hout.at[rows], dst_ref=h.at[0, rows], send_sem=h_send.at[r], recv_sem=h_recv.at[r],
            device_id=at(pipe_=lax.rem(pipe + 1, 4)), device_id_type=MESH,
        )

    def length_of(seq):
        return jnp.where(seq == 0, qlen[0], jnp.where(seq == 1, qlen[1], jnp.where(seq == 2, dlen[0], dlen[1])))

    length = length_of(z)
    lane = lax.broadcasted_iota(jnp.int32, (1, G), 1)
    head = lane // 64
    krow = lax.broadcasted_iota(jnp.int32, (G, 1), 0)
    one, zero = jnp.ones((), BF), jnp.zeros((), BF)

    @pl.loop(0, 4)
    def _(k):
        for r in range(nblk):

            @pl.when((first == 0) & (k == 2 * r))
            def _():
                hop_x(r).wait_recv()

        @pl.when((first == 1) & (k == 3))
        def _():
            step1()

        for v in range(2):
            u = 2 * k + v
            ahead = first * lax.rem(u // 2 + 1, 4)
            group = (1 - first) * lax.rem(u, 4)
            block = first * v + (1 - first) * (u // 4)
            rows = pl.ds(pl.multiple_of(block * 256, 256), 256)
            for i in range(3):
                scale = (0.125 * LOG2E, 1.0, VSCALE)[i]
                qkv[ahead + group, i, rows, :] = (dot(h[ahead, rows, :], b_qkv[group, i]) * scale).astype(BF)

    @pl.loop(0, 4)
    def _(g):
        kt[g] = qkv[g, 1].T

    def order_of(t):
        return lax.rem(2 + 3 * t + 3 * (t // 2) + 2 * (t // 3), 4)

    @pl.loop(0, 2 - first)
    def _(blk):
        @pl.loop(0, 2 + 2 * first)
        def _(t):
            @pl.when((first == 1) & (t == 1))
            def _():
                step2()
                for copy in share[2]:
                    copy.start()

            @pl.when((first == 1) & (t == 2))
            def _():
                for copy in share[1]:
                    copy.start()

            @pl.when((first == 1) & (t == 3))
            def _():
                for copy in share[3]:
                    copy.start()
                step3()

            ahead = order_of(t)
            for v in range(2):
                group = first * ahead + (1 - first) * (2 * t + v)
                block = first * v + (1 - first) * blk
                rows = pl.ds(pl.multiple_of(block * 256, 256), 256)
                for hd in range(4):
                    nxt = (hd + 1) % 4
                    mine, other, mark = head == hd, head == nxt, lane == nxt * 64
                    seq = lax.rem(z + first * ahead, 4)
                    bias = jnp.where(lax.broadcasted_iota(jnp.int32, (1, S), 1) < length_of(seq), 0.0, -1e30).astype(BF)
                    qm[v, hd] = jnp.where(mine, qkv[group, 0, rows, :], jnp.where(mark, one, zero))
                    km[v, hd] = jnp.where(krow == nxt * 64, bias, kt[group])
                    vm[v, hd] = jnp.where(mine, qkv[group, 2], jnp.where(other, one, zero))
            for hd in range(4):
                mine = head == hd
                for v in range(2):
                    p = jnp.exp2(dot(qm[v, hd], km[v, hd])).astype(BF)
                    o = dot(p, vm[v, hd])
                    total = pltpu.roll(o, 192, 1)
                    scale = jnp.where(total > 2.0**60, 2.0**-64, 1.0).astype(F32)
                    c = (o * scale) * (1.0 / (total * scale)) * (1.0 / VSCALE)
                    cf[v] = jnp.where(mine, c, cf[v] if hd else c)
            for v in range(2):
                group = first * (ahead + 4 * ((ahead + 3) // 4)) + (1 - first) * (2 * t + v)
                block = first * v + (1 - first) * blk
                ctx[group, pl.ds(pl.multiple_of(block * 256, 256), 256), :] = cf[v].astype(BF)

        @pl.when(first == 1)
        def _():
            step4()
            for here, on in zip(share[2], share_on):
                here.wait_recv()
                on.start()
            step5()
            for copy in (*share[1], *share[3], *share_on):
                copy.wait_recv()

        @pl.loop(0, 1 + first)
        def _(b):
            base = (blk + b) * 256
            rows = pl.ds(pl.multiple_of(base, 256), 256)
            for n in range(4):
                cs = slice(n * 256, (n + 1) * 256)
                acc[rows, cs] = sum(dot(ctx[j, rows, :], b_out[j, :, cs]) for j in range(4))

            @pl.loop(0, 4)
            def _(q):
                for u in range(2):
                    rr = pl.ds(pl.multiple_of(base + q * 64 + u * 32, 32), 32)
                    mixed[rr, :] = norm_rows(h[0, rr, :].astype(F32) + acc[rr, :], tile[0:1, :]).astype(BF)

        @pl.loop(0, 4 + 4 * first)
        def _(i):
            j = first * (i // 2) + (1 - first) * i
            r = first * lax.rem(i, 2) + (1 - first) * blk

            @pl.when((first == 1) & (i == 0))
            def _():
                step6()

            @pl.when((first == 1) & (i == 2))
            def _():
                step7()

            @pl.when((first == 1) & (i == 6))
            def _():
                step8()

            rows = pl.ds(pl.multiple_of(r * HALF, HALF), HALF)
            for n in range(4):
                cs = slice(n * 256, (n + 1) * 256)
                act[:, cs] = gelu(dot(mixed[rows, :], b_up[j, :, cs])).astype(BF)
            for n in range(4):
                cs = slice(n * 256, (n + 1) * 256)
                part = dot(act[...], b_down[j, :, cs])
                acc[rows, cs] = jnp.where(j == 0, part, acc[rows, cs] + part)

            @pl.when(j == 3)
            def _():
                @pl.loop(0, 4)
                def _(q):
                    for u in range(2):
                        rr = pl.ds(pl.multiple_of(r * HALF + q * 64 + u * 32, 32), 32)
                        hout[rr, :] = norm_rows(mixed[rr, :].astype(F32) + acc[rr, :], tile[8:9, :]).astype(BF)

                for rs in range(nblk):

                    @pl.when((pipe < 3) & (r == rs))
                    def _():
                        hop_x(rs).start()

    def t1(k):
        return pltpu.make_async_remote_copy(
            src_ref=dtab.at[z_low, dp], dst_ref=dtab.at[z_low, dp], send_sem=t1_send.at[k - 1], recv_sem=t1_recv.at[k - 1],
            device_id=at(dp_=lax.rem(dp + k, 8)), device_id_type=MESH,
        )

    def t1_in(k):
        there = lax.rem(dp + 8 - k, 8)
        return pltpu.make_async_remote_copy(
            src_ref=dtab.at[z_low, there], dst_ref=dtab.at[z_low, there], send_sem=t1_send.at[k - 1], recv_sem=t1_recv.at[k - 1],
            device_id=at(dp_=lax.rem(dp + k, 8)), device_id_type=MESH,
        )

    def t2(tab, slot, k):
        return pltpu.make_async_remote_copy(
            src_ref=tab.at[slot], dst_ref=tab.at[slot], send_sem=t2_send.at[k - 1], recv_sem=t2_recv.at[k - 1],
            device_id=at(z_=lax.rem(z + k, 4)), device_id_type=MESH,
        )

    def t3(k):
        return pltpu.make_async_remote_copy(
            src_ref=pieces.at[k], dst_ref=pieces.at[4], send_sem=t3_send.at[k], recv_sem=t3_recv.at[0], device_id=at(pipe_=k), device_id_type=MESH
        )

    @pl.when(pipe < 3)
    def _():
        t3(0).wait_recv()

    @pl.when(pipe == 3)
    def _():
        acc[0:8, :] = jnp.zeros((8, D), F32)

        @pl.loop(0, 16)
        def _(r):
            rows = pl.ds(pl.multiple_of(r * 32, 32), 32)
            keep = lax.broadcasted_iota(jnp.int32, (32, 1), 0) + r * 32 < length
            x = jnp.where(keep, hout[rows, :].astype(F32), 0.0)
            acc[0:8, :] += x[0:8] + x[8:16] + x[16:24] + x[24:32]

        pooled = jnp.sum(acc[0:8, :], axis=0, keepdims=True) / length.astype(F32)
        emb = pooled * lax.rsqrt(jnp.sum(pooled * pooled, axis=-1, keepdims=True) + 1e-6)
        emb = emb.astype(BF).astype(F32)

        @pl.when(z < 2)
        def _():
            for k in range(8):
                qtab[z_low, k : k + 1, :] = emb[:, k * 128 : (k + 1) * 128]

        @pl.when(z >= 2)
        def _():
            for k in range(8):
                dtab[z_low, dp, k : k + 1, :] = emb[:, k * 128 : (k + 1) * 128]
            for k in range(1, 8):
                t1(k).start()
            for k in range(1, 8):
                t1_in(k).wait_recv()
            for k in range(1, 4):
                t2(dtab, z_low, k).start()

        @pl.when(z < 2)
        def _():
            for k in range(1, 4):
                t2(qtab, z_low, k).start()

        for k in range(1, 4):
            there = lax.rem(z + 4 - k, 4)

            @pl.when(there < 2)
            def _():
                t2(qtab, lax.rem(there, 2), k).wait_recv()

            @pl.when(there >= 2)
            def _():
                t2(dtab, lax.rem(there, 2), k).wait_recv()

        doc_dp = lax.broadcasted_iota(jnp.int32, (8, 1), 0)
        losses = []
        for i in range(2):
            total, positive = jnp.zeros((1, 1), F32), jnp.zeros((1, 1), F32)
            for s in range(2):
                prod = dtab[s] * qtab[i][None]
                score = jnp.sum(jnp.sum(prod, axis=1), axis=1, keepdims=True) / 0.05
                total += jnp.sum(jnp.exp(score), axis=0, keepdims=True)
                hit = (doc_dp == dp) & (order[0, i] == s)
                positive += jnp.sum(jnp.where(hit, score, 0.0), axis=0, keepdims=True)
            losses.append(jnp.broadcast_to(jnp.log(total) - positive, (1, 128)))
        for k in (0, 1, 2, 3):
            row = 2 * k + z // 2
            pieces[k, 6:8, :] = jnp.zeros((2, 128), F32)
            for i in range(2):
                for at_row, line in ((i, qtab[i, pl.ds(row, 1), :]), (2 + i, dtab[i, dp, pl.ds(row, 1), :])):
                    pieces[k, at_row : at_row + 1, :] = jnp.where(z_low == 0, line, pltpu.roll(line, 64, 1))
                pieces[k, 4 + i : 5 + i, :] = losses[i]
            if k < 3:
                t3(k).start()
        pieces[4] = pieces[3]

    out[...] = pieces[4]

    for table in (hop1, hop2, yhop1, yhop2, d2d):
        for key, copy in table.items():
            if key[0] != "qkv":
                copy.wait_send()

    @pl.when(first == 0)
    def _():
        for table in (hop1, hop2, d2d):
            for key, copy in table.items():
                if key[0] == "qkv":
                    copy.wait_send()

    @pl.when(first == 1)
    def _():
        for copy in (*share[1], *share[2], *share[3], *share_on):
            copy.wait_send()

    @pl.when(pipe < 3)
    def _():
        for r in range(nblk):
            hop_x(r).wait_send()

    @pl.when(pipe == 3)
    def _():
        for k in range(3):
            t3(k).wait_send()

        @pl.when(z >= 2)
        def _():
            for k in range(1, 8):
                t1(k).wait_send()
            for k in range(1, 4):
                t2(dtab, z_low, k).wait_send()

        @pl.when(z < 2)
        def _():
            for k in range(1, 4):
                t2(qtab, z_low, k).wait_send()


def per_device(query_states, doc_states, query_len, doc_len, doc_order, w_qkv, w_out, w_up, w_down, gain_attn, gain_mlp):
    anyspace = pl.BlockSpec(memory_space=pl.ANY)
    smem = pl.BlockSpec(memory_space=pltpu.SMEM)
    vmem = pl.BlockSpec(memory_space=pltpu.VMEM)
    out = pl.pallas_call(
        kernel,
        out_shape=jax.ShapeDtypeStruct((8, 128), F32),
        in_specs=[anyspace, anyspace, smem, smem, smem, *[anyspace] * 6],
        out_specs=vmem,
        scratch_shapes=[
            pltpu.VMEM((4, 3, D, G), BF),
            pltpu.VMEM((4, G, D), BF),
            pltpu.VMEM((4, D, D), BF),
            pltpu.VMEM((4, D, D), BF),
            pltpu.VMEM((4, S, D), BF),
            pltpu.VMEM((S, D), BF),
            pltpu.VMEM((4, 3, S, G), BF),
            pltpu.VMEM((2, 4, 256, G), BF),
            pltpu.VMEM((2, 4, G, S), BF),
            pltpu.VMEM((4, G, S), BF),
            pltpu.VMEM((2, 4, S, G), BF),
            pltpu.VMEM((2, 256, G), F32),
            pltpu.VMEM((8, S, G), BF),
            pltpu.VMEM((2, 256, G), BF),
            pltpu.VMEM((S, D), F32),
            pltpu.VMEM((S, D), BF),
            pltpu.VMEM((HALF, D), BF),
            pltpu.VMEM((2, 8, 128), F32),
            pltpu.VMEM((2, 8, 8, 128), F32),
            pltpu.VMEM((5, 8, 128), F32),
            pltpu.VMEM((16, D), F32),
            pltpu.SemaphoreType.DMA((N_SEMS,)),
            pltpu.SemaphoreType.DMA((N_SEMS,)),
            pltpu.SemaphoreType.DMA((12,)),
            pltpu.SemaphoreType.DMA((6,)),
            pltpu.SemaphoreType.DMA((6,)),
            pltpu.SemaphoreType.DMA((S // HALF,)),
            pltpu.SemaphoreType.DMA((S // HALF,)),
            pltpu.SemaphoreType.DMA((7,)),
            pltpu.SemaphoreType.DMA((7,)),
            pltpu.SemaphoreType.DMA((3,)),
            pltpu.SemaphoreType.DMA((3,)),
            pltpu.SemaphoreType.DMA((3,)),
            pltpu.SemaphoreType.DMA((1,)),
        ],
        compiler_params=pltpu.CompilerParams(collective_id=0, has_side_effects=True, vmem_limit_bytes=63 * 2**20),
        name="encode",
    )(query_states, doc_states, query_len, doc_len, doc_order, w_qkv, w_out, w_up, w_down, gain_attn, gain_mlp)
    return out[0:2, :64].astype(BF), out[2:4, :64].astype(BF), out[4:6, 0]


def solution(mesh):
    in_specs = (
        P("dp", None, None),
        P("dp", None, None),
        P("dp"),
        P("dp"),
        P("dp", None),
        P("pipe", None, None, "tensor"),
        P("pipe", "tensor", None),
        P("pipe", None, "tensor"),
        P("pipe", "tensor", None),
        P("pipe", None),
        P("pipe", None),
    )
    out_specs = (P("dp", ("pipe", "tensor")), P("dp", ("pipe", "tensor")), P("dp"))
    return jax.shard_map(per_device, mesh=mesh, in_specs=in_specs, out_specs=out_specs, check_vma=False)
```

```python
import jax
import jax.numpy as jnp
from jax import lax
from jax.experimental import pallas as pl
from jax.experimental.pallas import tpu as pltpu
from jax.sharding import PartitionSpec as P

S = 512
D = 1024
G = 256
HALF = 256
DIRECT = 176
CHUNKS = ((176, 48), (224, 32))
BF = jnp.bfloat16
F32 = jnp.float32
LOG2E = 1.4426950408889634
VSCALE = 2.0**-14
SQRT_HALF = 0.7071067811865476
MESH = pl.DeviceIdType.MESH
ARRAYS = ("qkv", "out", "up", "down")
MLP = ("up", "down")
depth_half = {"qkv": 512, "out": 128, "up": 512, "down": 512}


def dot(a, b):
    return jnp.dot(a, b, preferred_element_type=F32)


def norm_rows(x, gain):
    mean = jnp.mean(x, axis=-1, keepdims=True)
    centered = x - mean
    variance = jnp.mean(centered * centered, axis=-1, keepdims=True)
    return centered * lax.rsqrt(variance + 1e-12) * gain


def gelu(u):
    return 0.5 * u * (1.0 + lax.erf(u * SQRT_HALF))


class Sems:
    def __init__(self, send, recv):
        self.send, self.recv, self.used = send, recv, 0

    def remote(self, src, dst, device):
        i = self.used
        self.used += 1
        return pltpu.make_async_remote_copy(
            src_ref=src, dst_ref=dst, send_sem=self.send.at[i], recv_sem=self.recv.at[i], device_id=device, device_id_type=MESH
        )


    def again(self, i, ref, device):
        return pltpu.make_async_remote_copy(
            src_ref=ref, dst_ref=ref, send_sem=self.send.at[i], recv_sem=self.recv.at[i], device_id=device, device_id_type=MESH
        )


N_SEMS = 60


def kernel(
    states_q, states_d, qlen, dlen, order, w_qkv, w_out, w_up, w_down, gain_attn, gain_mlp,
    out,
    b_qkv, b_out, b_up, b_down, h, hout, qkv, qm, km, kt, vm, cf, tf, ctx, relay, hrelay, acc, mixed, act, qtab, dtab, pieces, tile,
    send, recv, local, c_send, c_recv, h_send, h_recv, w_send, w_recv, t1_send, t1_recv, t2_send, t2_recv, t3_send, t3_recv,
):
    dp, pipe, z = lax.axis_index("dp"), lax.axis_index("pipe"), lax.axis_index("tensor")
    core = lax.rem(dp, 2)
    first = 1 - (pipe + 3) // 4

    def at(dp_=dp, pipe_=pipe, z_=z):
        return (dp_, pipe_, z_)

    up_z, down_z = at(z_=lax.rem(z + 1, 4)), at(z_=lax.rem(z + 3, 4))
    sibling = at(dp_=dp + 1 - 2 * core)

    barrier = pltpu.get_barrier_semaphore()
    for k in range(1, 8):
        pl.semaphore_signal(barrier, inc=1, device_id=at(dp_=lax.rem(dp + k, 8)), device_id_type=MESH)
    for k in range(1, 4):
        pl.semaphore_signal(barrier, inc=1, device_id=at(pipe_=lax.rem(pipe + k, 4)), device_id_type=MESH)
        pl.semaphore_signal(barrier, inc=1, device_id=at(z_=lax.rem(z + k, 4)), device_id_type=MESH)

    y = dp // 2
    own = {"qkv": w_qkv, "out": w_out, "up": w_up, "down": w_down}
    full = {"qkv": b_qkv, "out": b_out, "up": b_up, "down": b_down}
    north, south = at(dp_=lax.rem(dp + 2, 8)), at(dp_=lax.rem(dp + 6, 8))

    def window(name, ref, start, size):
        sl = pl.ds(pl.multiple_of(start, 16), size)
        return ref.at[:, sl, :] if name == "qkv" else ref.at[sl, :]

    def quarter(k):
        return core * 512 + 128 + 96 * lax.rem(y + k + 4, 4)

    parts = {
        "qkv": {"Z": (core * 512, 512)},
        "out": {"Z": (core * 128, 128)},
        "up": {"Z": (core * 512, 128), "Q": (quarter(0), 96)},
        "down": {"Z": (core * 512, 128), "Q": (quarter(0), 96)},
    }
    sems = Sems(send, recv)
    hop1, hop2, yhop1, yin1, yhop2, yin2, d2d = {}, {}, {}, {}, {}, {}, {}
    for name in ARRAYS:
        buf = full[name]
        for part, (start, size) in parts[name].items():
            src = window(name, own[name].at[0], start, size)
            hop1[name, part, 1] = sems.remote(src, window(name, buf.at[1], start, size), up_z)
            hop1[name, part, 2] = sems.remote(src, window(name, buf.at[2], start, size), down_z)
            half = size // 2
            a, b = (start, half), (start + half, half)
            hop2[name, part, "a"] = sems.remote(window(name, buf.at[1], *a), window(name, buf.at[3], *a), up_z)
            hop2[name, part, "b"] = sems.remote(window(name, buf.at[2], *b), window(name, buf.at[3], *b), down_z)
        for slot in (1, 2, 3):
            size = depth_half[name]
            mine = window(name, buf.at[slot], core * size, size)
            d2d[name, slot] = sems.remote(mine, mine, sibling)
    for name in MLP:
        for slot in (1, 2, 3):
            buf = full[name].at[slot]

            def part(k, first_row=0, size=96, buf=buf, name=name):
                return window(name, buf, quarter(k) + first_row, size)

            for sign, to in ((1, north), (-1, south)):
                i = sems.used
                yhop1[name, slot, sign] = sems.remote(part(0), part(0), to)
                yin1[name, slot, sign] = sems.again(i, part(-sign), to)
                row = 0 if sign == 1 else 48
                i = sems.used
                yhop2[name, slot, sign] = sems.remote(part(-sign, row, 48), part(-sign, row, 48), to)
                yin2[name, slot, sign] = sems.again(i, part(2, row, 48), to)
    loads = {name: pltpu.make_async_copy(own[name].at[0], full[name].at[0], local.at[i]) for i, name in enumerate(ARRAYS)}

    def begin(name, part):
        hop1[name, part, 1].start()
        hop1[name, part, 2].start()

    def z_near(name, part):
        hop1[name, part, 1].wait_recv()
        hop2[name, part, "a"].start()
        hop1[name, part, 2].wait_recv()
        hop2[name, part, "b"].start()

    def z_far(name, part):
        hop2[name, part, "a"].wait_recv()
        hop2[name, part, "b"].wait_recv()

    def y_begin(name, *slots):
        for slot in slots:
            for sign in (1, -1):
                yhop1[name, slot, sign].start()

    def y_on(name, *slots):
        for slot in slots:
            for sign in (1, -1):
                yin1[name, slot, sign].wait_recv()
                yhop2[name, slot, sign].start()

    def y_end(name, *slots):
        for slot in slots:
            for sign in (1, -1):
                yin2[name, slot, sign].wait_recv()
            d2d[name, slot].start()

    def arrive(name, *slots):
        for slot in slots:
            d2d[name, slot].wait_recv()

    def give(name, *slots):
        for slot in slots:
            d2d[name, slot].start()

    def begin_all():
        begin("out", "Z")
        begin("up", "Q")
        begin("down", "Q")

    def step1():
        z_near("out", "Z")
        give("out", 1, 2)

    def step2():
        z_near("up", "Q")
        y_begin("up", 1, 2)

    def step3():
        z_near("down", "Q")
        y_begin("down", 1, 2)

    def step4():
        z_far("out", "Z")
        give("out", 3)
        z_far("up", "Q")
        y_begin("up", 3)
        y_on("up", 1, 2)

    def step5():
        begin("up", "Z")
        begin("down", "Z")
        y_on("down", 1, 2)
        z_far("down", "Q")
        y_begin("down", 3)
        arrive("out", 1, 2, 3)

    def step6():
        y_on("up", 3)

    def step7():
        z_near("up", "Z")
        y_end("up", 1, 2)
        y_on("down", 3)
        z_near("down", "Z")
        y_end("down", 1, 2)
        arrive("up", 1, 2)
        arrive("down", 1, 2)

    def step8():
        z_far("up", "Z")
        y_end("up", 3)
        z_far("down", "Z")
        y_end("down", 3)
        arrive("up", 3)
        arrive("down", 3)

    loads["qkv"].start()
    gains = [pltpu.make_async_copy(gain_attn, tile.at[pl.ds(0, 1)], local.at[4]), pltpu.make_async_copy(gain_mlp, tile.at[pl.ds(8, 1)], local.at[5])]
    for g in gains:
        g.start()

    def input_copy(ref, index, k):
        return pltpu.make_async_copy(ref.at[index], h.at[k], local.at[8 + k])

    @pl.when(first == 1)
    def _():
        for k in range(4):
            seq = lax.rem(z + k, 4)

            @pl.when(seq < 2)
            def _():
                input_copy(states_q, lax.rem(seq, 2), k).start()

            @pl.when(seq >= 2)
            def _():
                input_copy(states_d, lax.rem(seq, 2), k).start()

    for name in ("out", *MLP):
        loads[name].start()
    pl.semaphore_wait(barrier, 13)
    begin_all()
    nblk = S // HALF

    def hop_x(r, size=HALF):
        rows = pl.ds(r * HALF, size)
        return pltpu.make_async_remote_copy(
            src_ref=hout.at[rows], dst_ref=h.at[0, rows], send_sem=h_send.at[r], recv_sem=h_recv.at[r],
            device_id=at(pipe_=lax.rem(pipe + 1, 4)), device_id_type=MESH,
        )

    chunks = [(r, c) for r in range(nblk) for c in range(len(CHUNKS))]

    def way_round(r, c, src, dst):
        start, size = CHUNKS[c]
        here, there = pl.ds(r * HALF + start, size), pl.ds(r * (HALF - DIRECT) + start - DIRECT, size)
        pick = {"out": hout.at[here], "relay": hrelay.at[there], "in": h.at[0, here]}
        return pltpu.make_async_remote_copy(
            src_ref=pick[src], dst_ref=pick[dst], send_sem=w_send.at[r * len(CHUNKS) + c], recv_sem=w_recv.at[r * len(CHUNKS) + c],
            device_id=at(pipe_=lax.rem(pipe + 3, 4)), device_id_type=MESH,
        )

    def send_on(r):
        @pl.when(first == 1)
        def _():
            for c in range(len(CHUNKS)):
                way_round(r, c, "out", "relay").start()
            hop_x(r, DIRECT).start()

        @pl.when((pipe == 1) | (pipe == 2))
        def _():
            hop_x(r).start()

    def take(r):
        @pl.when(pipe == 1)
        def _():
            hop_x(r, DIRECT).wait_recv()
            for c in range(len(CHUNKS)):
                way_round(r, c, "relay", "in").wait_recv()

        @pl.when(pipe >= 2)
        def _():
            hop_x(r).wait_recv()

    def pass_on():
        @pl.when(pipe == 3)
        def _():
            for r, c in chunks:
                way_round(r, c, "out", "relay").wait_recv()
                way_round(r, c, "relay", "relay").start()

        @pl.when(pipe == 2)
        def _():
            for r, c in chunks:
                way_round(r, c, "relay", "relay").wait_recv()
                way_round(r, c, "relay", "in").start()

    def sent():
        @pl.when(first == 1)
        def _():
            for r, c in chunks:
                way_round(r, c, "out", "relay").wait_send()
            for r in range(nblk):
                hop_x(r, DIRECT).wait_send()

        @pl.when((pipe == 1) | (pipe == 2))
        def _():
            for r in range(nblk):
                hop_x(r).wait_send()

        @pl.when(pipe == 3)
        def _():
            for r, c in chunks:
                way_round(r, c, "relay", "relay").wait_send()

        @pl.when(pipe == 2)
        def _():
            for r, c in chunks:
                way_round(r, c, "relay", "in").wait_send()

    z_low = lax.rem(z, 2)

    @pl.when(first == 0)
    def _():
        step1()
        step2()
        begin("qkv", "Z")
        step3()
        step4()
        step5()
        z_near("qkv", "Z")
        give("qkv", 1, 2)
        step6()
        step7()
        pass_on()
        z_far("qkv", "Z")
        give("qkv", 3)
        step8()
        arrive("qkv", 1, 2, 3)

    loads["qkv"].wait()

    @pl.when(first == 1)
    def _():
        for k in range(4):
            input_copy(states_q, 0, k).wait()

    def to_z(i, src, dst, k):
        return pltpu.make_async_remote_copy(
            src_ref=src, dst_ref=dst, send_sem=c_send.at[i], recv_sem=c_recv.at[i], device_id=at(z_=lax.rem(z + k, 4)), device_id_type=MESH
        )

    top, bottom = pl.ds(0, 256), pl.ds(256, 256)
    share = {
        1: (to_z(0, ctx.at[5], ctx.at[1], 1),),
        3: (to_z(1, ctx.at[7], ctx.at[2], 3),),
        2: (to_z(2, ctx.at[6, top], relay.at[0], 1), to_z(3, ctx.at[6, bottom], relay.at[1], 3)),
    }
    share_on = (to_z(4, relay.at[0], ctx.at[3, top], 1), to_z(5, relay.at[1], ctx.at[3, bottom], 3))

    def length_of(seq):
        return jnp.where(seq == 0, qlen[0], jnp.where(seq == 1, qlen[1], jnp.where(seq == 2, dlen[0], dlen[1])))

    length = length_of(z)
    lane = lax.broadcasted_iota(jnp.int32, (1, G), 1)
    head = lane // 64
    krow = lax.broadcasted_iota(jnp.int32, (G, 1), 0)
    one, zero = jnp.ones((), BF), jnp.zeros((), BF)

    @pl.loop(0, 4)
    def _(k):
        for r in range(nblk):

            @pl.when((first == 0) & (k == 2 * r))
            def _():
                take(r)

        @pl.when((first == 1) & (k == 3))
        def _():
            step1()

        for v in range(2):
            u = 2 * k + v
            ahead = first * lax.rem(u // 2 + 1, 4)
            group = (1 - first) * lax.rem(u, 4)
            block = first * v + (1 - first) * (u // 4)
            rows = pl.ds(pl.multiple_of(block * 256, 256), 256)
            for i in range(3):
                scale = (0.125 * LOG2E, 1.0, VSCALE)[i]
                qkv[ahead + group, i, rows, :] = (dot(h[ahead, rows, :], b_qkv[group, i]) * scale).astype(BF)

    @pl.loop(0, 4)
    def _(g):
        kt[g] = qkv[g, 1].T

    for name in ("out", *MLP):
        loads[name].wait()
    for g in gains:
        g.wait()

    def order_of(t):
        return lax.rem(2 + 3 * t + 3 * (t // 2) + 2 * (t // 3), 4)

    @pl.loop(0, 2 - first)
    def _(blk):
        @pl.loop(0, 2 + 2 * first)
        def _(t):
            @pl.when((first == 1) & (t == 1))
            def _():
                step2()
                for copy in share[2]:
                    copy.start()

            @pl.when((first == 1) & (t == 2))
            def _():
                for copy in share[1]:
                    copy.start()

            @pl.when((first == 1) & (t == 3))
            def _():
                for copy in share[3]:
                    copy.start()
                step3()

            ahead = order_of(t)
            for v in range(2):
                group = first * ahead + (1 - first) * (2 * t + v)
                block = first * v + (1 - first) * blk
                rows = pl.ds(pl.multiple_of(block * 256, 256), 256)
                for hd in range(4):
                    nxt = (hd + 1) % 4
                    mine, other, mark = head == hd, head == nxt, lane == nxt * 64
                    seq = lax.rem(z + first * ahead, 4)
                    bias = jnp.where(lax.broadcasted_iota(jnp.int32, (1, S), 1) < length_of(seq), 0.0, -1e30).astype(BF)
                    qm[v, hd] = jnp.where(mine, qkv[group, 0, rows, :], jnp.where(mark, one, zero))
                    km[v, hd] = jnp.where(krow == nxt * 64, bias, kt[group])
                    vm[v, hd] = jnp.where(mine, qkv[group, 2], jnp.where(other, one, zero))
            for hd in range(4):
                mine = head == hd
                for v in range(2):
                    p = jnp.exp2(dot(qm[v, hd], km[v, hd])).astype(BF)
                    o = dot(p, vm[v, hd])
                    cf[v] = jnp.where(mine, o, cf[v]) if hd else o
                    tf[v] = jnp.where(head == (hd + 1) % 4, o, tf[v]) if hd else o
            for v in range(2):
                total = pltpu.roll(tf[v], 192, 1)
                scale = jnp.where(total > 2.0**60, 2.0**-64, 1.0).astype(F32)
                c = (cf[v] * scale) * (1.0 / (total * scale)) * (1.0 / VSCALE)
                group = first * (ahead + 4 * ((ahead + 3) // 4)) + (1 - first) * (2 * t + v)
                block = first * v + (1 - first) * blk
                ctx[group, pl.ds(pl.multiple_of(block * 256, 256), 256), :] = c.astype(BF)

        @pl.when(first == 1)
        def _():
            step4()
            for here, on in zip(share[2], share_on):
                here.wait_recv()
                on.start()
            step5()
            for copy in (*share[1], *share[3], *share_on):
                copy.wait_recv()

        @pl.loop(0, 1 + first)
        def _(b):
            base = (blk + b) * 256
            rows = pl.ds(pl.multiple_of(base, 256), 256)
            for n in range(4):
                cs = slice(n * 256, (n + 1) * 256)
                acc[rows, cs] = sum(dot(ctx[j, rows, :], b_out[j, :, cs]) for j in range(4))

            @pl.loop(0, 2)
            def _(q):
                for u in range(4):
                    rr = pl.ds(pl.multiple_of(base + q * 128 + u * 32, 32), 32)
                    mixed[rr, :] = norm_rows(h[0, rr, :].astype(F32) + acc[rr, :], tile[0:1, :]).astype(BF)

        @pl.loop(0, 4 + 4 * first)
        def _(i):
            j = first * (i // 2) + (1 - first) * i
            r = first * lax.rem(i, 2) + (1 - first) * blk

            @pl.when((first == 1) & (i == 0))
            def _():
                step6()

            @pl.when((first == 1) & (i == 2))
            def _():
                step7()

            @pl.when((first == 1) & (i == 6))
            def _():
                step8()

            rows = pl.ds(pl.multiple_of(r * HALF, HALF), HALF)
            for n in range(4):
                cs = slice(n * 256, (n + 1) * 256)
                act[:, cs] = gelu(dot(mixed[rows, :], b_up[j, :, cs])).astype(BF)
            for n in range(4):
                cs = slice(n * 256, (n + 1) * 256)
                part = dot(act[...], b_down[j, :, cs])
                acc[rows, cs] = jnp.where(j == 0, part, acc[rows, cs] + part)

            @pl.when(j == 3)
            def _():
                @pl.loop(0, 2)
                def _(q):
                    for u in range(4):
                        rr = pl.ds(pl.multiple_of(r * HALF + q * 128 + u * 32, 32), 32)
                        hout[rr, :] = norm_rows(mixed[rr, :].astype(F32) + acc[rr, :], tile[8:9, :]).astype(BF)

                for rs in range(nblk):

                    @pl.when((pipe < 3) & (r == rs))
                    def _():
                        send_on(rs)

    def t1(k):
        return pltpu.make_async_remote_copy(
            src_ref=dtab.at[z_low, dp], dst_ref=dtab.at[z_low, dp], send_sem=t1_send.at[k - 1], recv_sem=t1_recv.at[k - 1],
            device_id=at(dp_=lax.rem(dp + k, 8)), device_id_type=MESH,
        )

    def t1_in(k):
        there = lax.rem(dp + 8 - k, 8)
        return pltpu.make_async_remote_copy(
            src_ref=dtab.at[z_low, there], dst_ref=dtab.at[z_low, there], send_sem=t1_send.at[k - 1], recv_sem=t1_recv.at[k - 1],
            device_id=at(dp_=lax.rem(dp + k, 8)), device_id_type=MESH,
        )

    def t2(tab, slot, k):
        return pltpu.make_async_remote_copy(
            src_ref=tab.at[slot], dst_ref=tab.at[slot], send_sem=t2_send.at[k - 1], recv_sem=t2_recv.at[k - 1],
            device_id=at(z_=lax.rem(z + k, 4)), device_id_type=MESH,
        )

    def t3(k):
        return pltpu.make_async_remote_copy(
            src_ref=pieces.at[k], dst_ref=pieces.at[4], send_sem=t3_send.at[k], recv_sem=t3_recv.at[0], device_id=at(pipe_=k), device_id_type=MESH
        )

    @pl.when(pipe < 3)
    def _():
        t3(0).wait_recv()

    @pl.when(pipe == 3)
    def _():
        acc[0:8, :] = jnp.zeros((8, D), F32)

        @pl.loop(0, 16)
        def _(r):
            rows = pl.ds(pl.multiple_of(r * 32, 32), 32)
            keep = lax.broadcasted_iota(jnp.int32, (32, 1), 0) + r * 32 < length
            x = jnp.where(keep, hout[rows, :].astype(F32), 0.0)
            acc[0:8, :] += x[0:8] + x[8:16] + x[16:24] + x[24:32]

        pooled = jnp.sum(acc[0:8, :], axis=0, keepdims=True) / length.astype(F32)
        emb = pooled * lax.rsqrt(jnp.sum(pooled * pooled, axis=-1, keepdims=True) + 1e-6)
        emb = emb.astype(BF).astype(F32)

        @pl.when(z < 2)
        def _():
            for k in range(8):
                qtab[z_low, k : k + 1, :] = emb[:, k * 128 : (k + 1) * 128]

        @pl.when(z >= 2)
        def _():
            for k in range(8):
                dtab[z_low, dp, k : k + 1, :] = emb[:, k * 128 : (k + 1) * 128]
            for k in range(1, 8):
                t1(k).start()
            for k in range(1, 8):
                t1_in(k).wait_recv()
            for k in range(1, 4):
                t2(dtab, z_low, k).start()

        @pl.when(z < 2)
        def _():
            for k in range(1, 4):
                t2(qtab, z_low, k).start()

        for k in range(1, 4):
            there = lax.rem(z + 4 - k, 4)

            @pl.when(there < 2)
            def _():
                t2(qtab, lax.rem(there, 2), k).wait_recv()

            @pl.when(there >= 2)
            def _():
                t2(dtab, lax.rem(there, 2), k).wait_recv()

        doc_dp = lax.broadcasted_iota(jnp.int32, (8, 1), 0)
        losses = []
        for i in range(2):
            total, positive = jnp.zeros((1, 1), F32), jnp.zeros((1, 1), F32)
            for s in range(2):
                prod = dtab[s] * qtab[i][None]
                score = jnp.sum(jnp.sum(prod, axis=1), axis=1, keepdims=True) / 0.05
                total += jnp.sum(jnp.exp(score), axis=0, keepdims=True)
                hit = (doc_dp == dp) & (order[0, i] == s)
                positive += jnp.sum(jnp.where(hit, score, 0.0), axis=0, keepdims=True)
            losses.append(jnp.broadcast_to(jnp.log(total) - positive, (1, 128)))
        for k in (0, 1, 2, 3):
            row = 2 * k + z // 2
            pieces[k, 6:8, :] = jnp.zeros((2, 128), F32)
            for i in range(2):
                for at_row, line in ((i, qtab[i, pl.ds(row, 1), :]), (2 + i, dtab[i, dp, pl.ds(row, 1), :])):
                    pieces[k, at_row : at_row + 1, :] = jnp.where(z_low == 0, line, pltpu.roll(line, 64, 1))
                pieces[k, 4 + i : 5 + i, :] = losses[i]
            if k < 3:
                t3(k).start()
        pieces[4] = pieces[3]

    out[...] = pieces[4]

    for table in (hop1, hop2, yhop1, yhop2, d2d):
        for key, copy in table.items():
            if key[0] != "qkv":
                copy.wait_send()

    @pl.when(first == 0)
    def _():
        for table in (hop1, hop2, d2d):
            for key, copy in table.items():
                if key[0] == "qkv":
                    copy.wait_send()

    @pl.when(first == 1)
    def _():
        for copy in (*share[1], *share[2], *share[3], *share_on):
            copy.wait_send()

    sent()

    @pl.when(pipe == 3)
    def _():
        for k in range(3):
            t3(k).wait_send()

        @pl.when(z >= 2)
        def _():
            for k in range(1, 8):
                t1(k).wait_send()
            for k in range(1, 4):
                t2(dtab, z_low, k).wait_send()

        @pl.when(z < 2)
        def _():
            for k in range(1, 4):
                t2(qtab, z_low, k).wait_send()


def split(tile, out_q, out_d, out_loss):
    out_q[...] = tile[0:2, :64].astype(BF)
    out_d[...] = tile[2:4, :64].astype(BF)
    for i in range(2):
        out_loss[i] = tile[4 + i, 0]


def per_device(query_states, doc_states, query_len, doc_len, doc_order, w_qkv, w_out, w_up, w_down, gain_attn, gain_mlp):
    anyspace = pl.BlockSpec(memory_space=pl.ANY)
    smem = pl.BlockSpec(memory_space=pltpu.SMEM)
    vmem = pl.BlockSpec(memory_space=pltpu.VMEM)
    out = pl.pallas_call(
        kernel,
        out_shape=jax.ShapeDtypeStruct((8, 128), F32),
        in_specs=[anyspace, anyspace, smem, smem, smem, *[anyspace] * 6],
        out_specs=vmem,
        scratch_shapes=[
            pltpu.VMEM((4, 3, D, G), BF),
            pltpu.VMEM((4, G, D), BF),
            pltpu.VMEM((4, D, D), BF),
            pltpu.VMEM((4, D, D), BF),
            pltpu.VMEM((4, S, D), BF),
            pltpu.VMEM((S, D), BF),
            pltpu.VMEM((4, 3, S, G), BF),
            pltpu.VMEM((2, 4, 256, G), BF),
            pltpu.VMEM((2, 4, G, S), BF),
            pltpu.VMEM((4, G, S), BF),
            pltpu.VMEM((2, 4, S, G), BF),
            pltpu.VMEM((2, 256, G), F32),
            pltpu.VMEM((2, 256, G), F32),
            pltpu.VMEM((8, S, G), BF),
            pltpu.VMEM((2, 256, G), BF),
            pltpu.VMEM((2 * (HALF - DIRECT), D), BF),
            pltpu.VMEM((S, D), F32),
            pltpu.VMEM((S, D), BF),
            pltpu.VMEM((HALF, D), BF),
            pltpu.VMEM((2, 8, 128), F32),
            pltpu.VMEM((2, 8, 8, 128), F32),
            pltpu.VMEM((5, 8, 128), F32),
            pltpu.VMEM((16, D), F32),
            pltpu.SemaphoreType.DMA((N_SEMS,)),
            pltpu.SemaphoreType.DMA((N_SEMS,)),
            pltpu.SemaphoreType.DMA((12,)),
            pltpu.SemaphoreType.DMA((6,)),
            pltpu.SemaphoreType.DMA((6,)),
            pltpu.SemaphoreType.DMA((S // HALF,)),
            pltpu.SemaphoreType.DMA((S // HALF,)),
            pltpu.SemaphoreType.DMA((4,)),
            pltpu.SemaphoreType.DMA((4,)),
            pltpu.SemaphoreType.DMA((7,)),
            pltpu.SemaphoreType.DMA((7,)),
            pltpu.SemaphoreType.DMA((3,)),
            pltpu.SemaphoreType.DMA((3,)),
            pltpu.SemaphoreType.DMA((3,)),
            pltpu.SemaphoreType.DMA((1,)),
        ],
        compiler_params=pltpu.CompilerParams(collective_id=0, has_side_effects=True, vmem_limit_bytes=63 * 2**20),
        name="encode",
    )(query_states, doc_states, query_len, doc_len, doc_order, w_qkv, w_out, w_up, w_down, gain_attn, gain_mlp)
    return pl.pallas_call(
        split,
        out_shape=(jax.ShapeDtypeStruct((2, 64), BF), jax.ShapeDtypeStruct((2, 64), BF), jax.ShapeDtypeStruct((2,), F32)),
        in_specs=[vmem],
        out_specs=(vmem, vmem, smem),
        name="split",
    )(out)


def solution(mesh):
    in_specs = (
        P("dp", None, None),
        P("dp", None, None),
        P("dp"),
        P("dp"),
        P("dp", None),
        P("pipe", None, None, "tensor"),
        P("pipe", "tensor", None),
        P("pipe", None, "tensor"),
        P("pipe", "tensor", None),
        P("pipe", None),
        P("pipe", None),
    )
    out_specs = (P("dp", ("pipe", "tensor")), P("dp", ("pipe", "tensor")), P("dp"))
    return jax.shard_map(per_device, mesh=mesh, in_specs=in_specs, out_specs=out_specs, check_vma=False)
```

```python
import jax
import jax.numpy as jnp
from jax import lax
from jax.experimental import pallas as pl
from jax.experimental.pallas import tpu as pltpu
from jax.sharding import PartitionSpec as P

S = 512
D = 1024
G = 256
HALF = 256
DIRECT = 160
CHUNKS = ((160, 48), (208, 48))
BF = jnp.bfloat16
F32 = jnp.float32
LOG2E = 1.4426950408889634
VSCALE = 2.0**-14
SQRT_HALF = 0.7071067811865476
MESH = pl.DeviceIdType.MESH
ARRAYS = ("qkv", "out", "up", "down")
MLP = ("up", "down")
depth_half = {"qkv": 512, "out": 128, "up": 512, "down": 512}


def dot(a, b):
    return jnp.dot(a, b, preferred_element_type=F32)


def norm_rows(x, gain):
    mean = jnp.mean(x, axis=-1, keepdims=True)
    centered = x - mean
    variance = jnp.mean(centered * centered, axis=-1, keepdims=True)
    return centered * lax.rsqrt(variance + 1e-12) * gain


def gelu(u):
    return 0.5 * u * (1.0 + lax.erf(u * SQRT_HALF))


class Sems:
    def __init__(self, send, recv):
        self.send, self.recv, self.used = send, recv, 0

    def remote(self, src, dst, device):
        i = self.used
        self.used += 1
        return pltpu.make_async_remote_copy(
            src_ref=src, dst_ref=dst, send_sem=self.send.at[i], recv_sem=self.recv.at[i], device_id=device, device_id_type=MESH
        )


    def again(self, i, ref, device):
        return pltpu.make_async_remote_copy(
            src_ref=ref, dst_ref=ref, send_sem=self.send.at[i], recv_sem=self.recv.at[i], device_id=device, device_id_type=MESH
        )


N_SEMS = 60


def kernel(
    states_q, states_d, qlen, dlen, order, w_qkv, w_out, w_up, w_down, gain_attn, gain_mlp,
    out,
    b_qkv, b_out, b_up, b_down, h, hout, qkv, qm, km, kt, vm, cf, tf, ctx, relay, hrelay, acc, mixed, act, qtab, dtab, pieces, tile,
    send, recv, local, c_send, c_recv, h_send, h_recv, w_send, w_recv, t1_send, t1_recv, t2_send, t2_recv, t3_send, t3_recv,
):
    dp, pipe, z = lax.axis_index("dp"), lax.axis_index("pipe"), lax.axis_index("tensor")
    core = lax.rem(dp, 2)
    first = 1 - (pipe + 3) // 4

    def at(dp_=dp, pipe_=pipe, z_=z):
        return (dp_, pipe_, z_)

    up_z, down_z = at(z_=lax.rem(z + 1, 4)), at(z_=lax.rem(z + 3, 4))
    sibling = at(dp_=dp + 1 - 2 * core)

    barrier = pltpu.get_barrier_semaphore()
    for k in range(1, 8):
        pl.semaphore_signal(barrier, inc=1, device_id=at(dp_=lax.rem(dp + k, 8)), device_id_type=MESH)
    for k in range(1, 4):
        pl.semaphore_signal(barrier, inc=1, device_id=at(pipe_=lax.rem(pipe + k, 4)), device_id_type=MESH)
        pl.semaphore_signal(barrier, inc=1, device_id=at(z_=lax.rem(z + k, 4)), device_id_type=MESH)

    y = dp // 2
    own = {"qkv": w_qkv, "out": w_out, "up": w_up, "down": w_down}
    full = {"qkv": b_qkv, "out": b_out, "up": b_up, "down": b_down}
    north, south = at(dp_=lax.rem(dp + 2, 8)), at(dp_=lax.rem(dp + 6, 8))

    def window(name, ref, start, size):
        sl = pl.ds(pl.multiple_of(start, 16), size)
        return ref.at[:, sl, :] if name == "qkv" else ref.at[sl, :]

    def quarter(k):
        return core * 512 + 128 + 96 * lax.rem(y + k + 4, 4)

    parts = {
        "qkv": {"Z": (core * 512, 512)},
        "out": {"Z": (core * 128, 128)},
        "up": {"Z": (core * 512, 128), "Q": (quarter(0), 96)},
        "down": {"Z": (core * 512, 128), "Q": (quarter(0), 96)},
    }
    sems = Sems(send, recv)
    hop1, hop2, yhop1, yin1, yhop2, yin2, d2d = {}, {}, {}, {}, {}, {}, {}
    for name in ARRAYS:
        buf = full[name]
        for part, (start, size) in parts[name].items():
            src = window(name, own[name].at[0], start, size)
            hop1[name, part, 1] = sems.remote(src, window(name, buf.at[1], start, size), up_z)
            hop1[name, part, 2] = sems.remote(src, window(name, buf.at[2], start, size), down_z)
            half = size // 2
            a, b = (start, half), (start + half, half)
            hop2[name, part, "a"] = sems.remote(window(name, buf.at[1], *a), window(name, buf.at[3], *a), up_z)
            hop2[name, part, "b"] = sems.remote(window(name, buf.at[2], *b), window(name, buf.at[3], *b), down_z)
        for slot in (1, 2, 3):
            size = depth_half[name]
            mine = window(name, buf.at[slot], core * size, size)
            d2d[name, slot] = sems.remote(mine, mine, sibling)
    for name in MLP:
        for slot in (1, 2, 3):
            buf = full[name].at[slot]

            def part(k, first_row=0, size=96, buf=buf, name=name):
                return window(name, buf, quarter(k) + first_row, size)

            for sign, to in ((1, north), (-1, south)):
                i = sems.used
                yhop1[name, slot, sign] = sems.remote(part(0), part(0), to)
                yin1[name, slot, sign] = sems.again(i, part(-sign), to)
                row = 0 if sign == 1 else 48
                i = sems.used
                yhop2[name, slot, sign] = sems.remote(part(-sign, row, 48), part(-sign, row, 48), to)
                yin2[name, slot, sign] = sems.again(i, part(2, row, 48), to)
    loads = {name: pltpu.make_async_copy(own[name].at[0], full[name].at[0], local.at[i]) for i, name in enumerate(ARRAYS)}

    def begin(name, part):
        hop1[name, part, 1].start()
        hop1[name, part, 2].start()

    def z_near(name, part):
        hop1[name, part, 1].wait_recv()
        hop2[name, part, "a"].start()
        hop1[name, part, 2].wait_recv()
        hop2[name, part, "b"].start()

    def z_far(name, part):
        hop2[name, part, "a"].wait_recv()
        hop2[name, part, "b"].wait_recv()

    def y_begin(name, *slots):
        for slot in slots:
            for sign in (1, -1):
                yhop1[name, slot, sign].start()

    def y_on(name, *slots):
        for slot in slots:
            for sign in (1, -1):
                yin1[name, slot, sign].wait_recv()
                yhop2[name, slot, sign].start()

    def y_end(name, *slots):
        for slot in slots:
            for sign in (1, -1):
                yin2[name, slot, sign].wait_recv()
            d2d[name, slot].start()

    def arrive(name, *slots):
        for slot in slots:
            d2d[name, slot].wait_recv()

    def give(name, *slots):
        for slot in slots:
            d2d[name, slot].start()

    def begin_all():
        begin("out", "Z")
        begin("up", "Q")
        begin("down", "Q")

    def step1():
        z_near("out", "Z")
        give("out", 1, 2)

    def step2():
        z_near("up", "Q")
        y_begin("up", 1, 2)

    def step3():
        z_near("down", "Q")
        y_begin("down", 1, 2)

    def step4():
        z_far("out", "Z")
        give("out", 3)
        z_far("up", "Q")
        y_begin("up", 3)
        y_on("up", 1, 2)

    def step5():
        begin("up", "Z")
        begin("down", "Z")
        y_on("down", 1, 2)
        z_far("down", "Q")
        y_begin("down", 3)
        arrive("out", 1, 2, 3)

    def step6():
        y_on("up", 3)

    def step7():
        z_near("up", "Z")
        y_end("up", 1, 2)
        y_on("down", 3)
        z_near("down", "Z")
        y_end("down", 1, 2)
        arrive("up", 1, 2)
        arrive("down", 1, 2)

    def step8():
        z_far("up", "Z")
        y_end("up", 3)
        z_far("down", "Z")
        y_end("down", 3)
        arrive("up", 3)
        arrive("down", 3)

    loads["qkv"].start()
    gains = [pltpu.make_async_copy(gain_attn, tile.at[pl.ds(0, 1)], local.at[4]), pltpu.make_async_copy(gain_mlp, tile.at[pl.ds(8, 1)], local.at[5])]
    for g in gains:
        g.start()

    def input_copy(ref, index, k):
        return pltpu.make_async_copy(ref.at[index], h.at[k], local.at[8 + k])

    @pl.when(first == 1)
    def _():
        for k in range(4):
            seq = lax.rem(z + k, 4)

            @pl.when(seq < 2)
            def _():
                input_copy(states_q, lax.rem(seq, 2), k).start()

            @pl.when(seq >= 2)
            def _():
                input_copy(states_d, lax.rem(seq, 2), k).start()

    for name in ("out", *MLP):
        loads[name].start()
    pl.semaphore_wait(barrier, 13)
    begin_all()
    nblk = S // HALF

    def hop_x(r, size=HALF):
        rows = pl.ds(r * HALF, size)
        return pltpu.make_async_remote_copy(
            src_ref=hout.at[rows], dst_ref=h.at[0, rows], send_sem=h_send.at[r], recv_sem=h_recv.at[r],
            device_id=at(pipe_=lax.rem(pipe + 1, 4)), device_id_type=MESH,
        )

    chunks = [(r, c) for r in range(nblk) for c in range(len(CHUNKS))]

    def way_round(r, c, src, dst):
        start, size = CHUNKS[c]
        here, there = pl.ds(r * HALF + start, size), pl.ds(r * (HALF - DIRECT) + start - DIRECT, size)
        pick = {"out": hout.at[here], "relay": hrelay.at[there], "in": h.at[0, here]}
        return pltpu.make_async_remote_copy(
            src_ref=pick[src], dst_ref=pick[dst], send_sem=w_send.at[r * len(CHUNKS) + c], recv_sem=w_recv.at[r * len(CHUNKS) + c],
            device_id=at(pipe_=lax.rem(pipe + 3, 4)), device_id_type=MESH,
        )

    def send_on(r):
        @pl.when(first == 1)
        def _():
            for c in range(len(CHUNKS)):
                way_round(r, c, "out", "relay").start()
            hop_x(r, DIRECT).start()

        @pl.when((pipe == 1) | (pipe == 2))
        def _():
            hop_x(r).start()

    def take(r):
        @pl.when(pipe == 1)
        def _():
            hop_x(r, DIRECT).wait_recv()
            for c in range(len(CHUNKS)):
                way_round(r, c, "relay", "in").wait_recv()

        @pl.when(pipe >= 2)
        def _():
            hop_x(r).wait_recv()

    def pass_on():
        @pl.when(pipe == 3)
        def _():
            for r, c in chunks:
                way_round(r, c, "out", "relay").wait_recv()
                way_round(r, c, "relay", "relay").start()

        @pl.when(pipe == 2)
        def _():
            for r, c in chunks:
                way_round(r, c, "relay", "relay").wait_recv()
                way_round(r, c, "relay", "in").start()

    def sent():
        @pl.when(first == 1)
        def _():
            for r, c in chunks:
                way_round(r, c, "out", "relay").wait_send()
            for r in range(nblk):
                hop_x(r, DIRECT).wait_send()

        @pl.when((pipe == 1) | (pipe == 2))
        def _():
            for r in range(nblk):
                hop_x(r).wait_send()

        @pl.when(pipe == 3)
        def _():
            for r, c in chunks:
                way_round(r, c, "relay", "relay").wait_send()

        @pl.when(pipe == 2)
        def _():
            for r, c in chunks:
                way_round(r, c, "relay", "in").wait_send()

    z_low = lax.rem(z, 2)

    @pl.when(first == 0)
    def _():
        step1()
        step2()
        begin("qkv", "Z")
        step3()
        step4()
        step5()
        z_near("qkv", "Z")
        give("qkv", 1, 2)
        step6()
        step7()
        pass_on()
        z_far("qkv", "Z")
        give("qkv", 3)
        step8()
        arrive("qkv", 1, 2, 3)

    loads["qkv"].wait()

    @pl.when(first == 1)
    def _():
        for k in range(4):
            input_copy(states_q, 0, k).wait()

    def to_z(i, src, dst, k):
        return pltpu.make_async_remote_copy(
            src_ref=src, dst_ref=dst, send_sem=c_send.at[i], recv_sem=c_recv.at[i], device_id=at(z_=lax.rem(z + k, 4)), device_id_type=MESH
        )

    top, bottom = pl.ds(0, 256), pl.ds(256, 256)
    share = {
        1: (to_z(0, ctx.at[5], ctx.at[1], 1),),
        3: (to_z(1, ctx.at[7], ctx.at[2], 3),),
        2: (to_z(2, ctx.at[6, top], relay.at[0], 1), to_z(3, ctx.at[6, bottom], relay.at[1], 3)),
    }
    share_on = (to_z(4, relay.at[0], ctx.at[3, top], 1), to_z(5, relay.at[1], ctx.at[3, bottom], 3))

    def length_of(seq):
        return jnp.where(seq == 0, qlen[0], jnp.where(seq == 1, qlen[1], jnp.where(seq == 2, dlen[0], dlen[1])))

    length = length_of(z)
    lane = lax.broadcasted_iota(jnp.int32, (1, G), 1)
    head = lane // 64
    krow = lax.broadcasted_iota(jnp.int32, (G, 1), 0)
    one, zero = jnp.ones((), BF), jnp.zeros((), BF)

    @pl.loop(0, 4)
    def _(k):
        for r in range(nblk):

            @pl.when((first == 0) & (k == 2 * r))
            def _():
                take(r)

        @pl.when((first == 1) & (k == 3))
        def _():
            step1()

        for v in range(2):
            u = 2 * k + v
            ahead = first * lax.rem(u // 2 + 1, 4)
            group = (1 - first) * lax.rem(u, 4)
            block = first * v + (1 - first) * (u // 4)
            rows = pl.ds(pl.multiple_of(block * 256, 256), 256)
            for i in range(3):
                scale = (0.125 * LOG2E, 1.0, VSCALE)[i]
                qkv[ahead + group, i, rows, :] = (dot(h[ahead, rows, :], b_qkv[group, i]) * scale).astype(BF)

    @pl.loop(0, 4)
    def _(g):
        kt[g] = qkv[g, 1].T

    for name in ("out", *MLP):
        loads[name].wait()
    for g in gains:
        g.wait()

    def order_of(t):
        return lax.rem(2 + 3 * t + 3 * (t // 2) + 2 * (t // 3), 4)

    both = 1 - lax.rem((pipe + 1) // 2, 2)

    @pl.loop(0, 2 - both)
    def _(blk):
        @pl.loop(0, 2 + 2 * both)
        def _(t):
            @pl.when((first == 1) & (t == 1))
            def _():
                step2()
                for copy in share[2]:
                    copy.start()

            @pl.when((first == 1) & (t == 2))
            def _():
                for copy in share[1]:
                    copy.start()

            @pl.when((first == 1) & (t == 3))
            def _():
                for copy in share[3]:
                    copy.start()
                step3()

            ahead = order_of(t)
            for v in range(2):
                group = first * ahead + (1 - first) * (2 * lax.rem(t, 2) + v)
                block = first * v + (1 - first) * (blk + both * (t // 2))
                rows = pl.ds(pl.multiple_of(block * 256, 256), 256)
                for hd in range(4):
                    nxt = (hd + 1) % 4
                    mine, other, mark = head == hd, head == nxt, lane == nxt * 64
                    seq = lax.rem(z + first * ahead, 4)
                    bias = jnp.where(lax.broadcasted_iota(jnp.int32, (1, S), 1) < length_of(seq), 0.0, -1e30).astype(BF)
                    qm[v, hd] = jnp.where(mine, qkv[group, 0, rows, :], jnp.where(mark, one, zero))
                    km[v, hd] = jnp.where(krow == nxt * 64, bias, kt[group])
                    vm[v, hd] = jnp.where(mine, qkv[group, 2], jnp.where(other, one, zero))
            for hd in range(4):
                mine = head == hd
                for v in range(2):
                    p = jnp.exp2(dot(qm[v, hd], km[v, hd])).astype(BF)
                    o = dot(p, vm[v, hd])
                    cf[v] = jnp.where(mine, o, cf[v]) if hd else o
                    tf[v] = jnp.where(head == (hd + 1) % 4, o, tf[v]) if hd else o
            for v in range(2):
                total = pltpu.roll(tf[v], 192, 1)
                scale = jnp.where(total > 2.0**60, 2.0**-64, 1.0).astype(F32)
                c = (cf[v] * scale) * (1.0 / (total * scale)) * (1.0 / VSCALE)
                group = first * (ahead + 4 * ((ahead + 3) // 4)) + (1 - first) * (2 * lax.rem(t, 2) + v)
                block = first * v + (1 - first) * (blk + both * (t // 2))
                ctx[group, pl.ds(pl.multiple_of(block * 256, 256), 256), :] = c.astype(BF)

        @pl.when(first == 1)
        def _():
            step4()
            for here, on in zip(share[2], share_on):
                here.wait_recv()
                on.start()
            step5()
            for copy in (*share[1], *share[3], *share_on):
                copy.wait_recv()

        @pl.loop(0, 1 + both)
        def _(b):
            base = (blk + b) * 256
            rows = pl.ds(pl.multiple_of(base, 256), 256)
            for n in range(4):
                cs = slice(n * 256, (n + 1) * 256)
                acc[rows, cs] = sum(dot(ctx[j, rows, :], b_out[j, :, cs]) for j in range(4))

            for u in range(16):
                if True:
                    rr = pl.ds(pl.multiple_of(base + u * 16, 16), 16)
                    mixed[rr, :] = norm_rows(h[0, rr, :].astype(F32) + acc[rr, :], tile[0:1, :]).astype(BF)

        @pl.when(pipe == 3)
        def _():
            @pl.loop(0, 4)
            def _(j):
                for n in range(4):
                    cs = slice(n * 256, (n + 1) * 256)
                    act[:, cs] = gelu(dot(mixed[...], b_up[j, :, cs])).astype(BF)
                for n in range(4):
                    cs = slice(n * 256, (n + 1) * 256)
                    part = dot(act[...], b_down[j, :, cs])
                    acc[:, cs] = jnp.where(j == 0, part, acc[:, cs] + part)

            @pl.loop(0, 2)
            def _(q):
                for u in range(16):
                    rr = pl.ds(pl.multiple_of(q * 256 + u * 16, 16), 16)
                    hout[rr, :] = norm_rows(mixed[rr, :].astype(F32) + acc[rr, :], tile[8:9, :]).astype(BF)

        @pl.when(pipe < 3)
        def _():
            @pl.loop(0, 4 + 4 * first)
            def _(i):
                j = first * (i // 2) + (1 - first) * i
                r = first * lax.rem(i, 2) + (1 - first) * blk

                @pl.when((first == 1) & (i == 0))
                def _():
                    step6()

                @pl.when((first == 1) & (i == 2))
                def _():
                    step7()

                @pl.when((first == 1) & (i == 6))
                def _():
                    step8()

                rows = pl.ds(pl.multiple_of(r * HALF, HALF), HALF)
                for n in range(4):
                    cs = slice(n * 256, (n + 1) * 256)
                    act[:HALF, cs] = gelu(dot(mixed[rows, :], b_up[j, :, cs])).astype(BF)
                for n in range(4):
                    cs = slice(n * 256, (n + 1) * 256)
                    part = dot(act[:HALF, :], b_down[j, :, cs])
                    acc[rows, cs] = jnp.where(j == 0, part, acc[rows, cs] + part)

                @pl.when(j == 3)
                def _():
                    for u in range(16):
                        if True:
                            rr = pl.ds(pl.multiple_of(r * HALF + u * 16, 16), 16)
                            hout[rr, :] = norm_rows(mixed[rr, :].astype(F32) + acc[rr, :], tile[8:9, :]).astype(BF)

                    for rs in range(nblk):

                        @pl.when((pipe < 3) & (r == rs))
                        def _():
                            send_on(rs)

    def t1(k):
        return pltpu.make_async_remote_copy(
            src_ref=dtab.at[z_low, dp], dst_ref=dtab.at[z_low, dp], send_sem=t1_send.at[k - 1], recv_sem=t1_recv.at[k - 1],
            device_id=at(dp_=lax.rem(dp + k, 8)), device_id_type=MESH,
        )

    def t1_in(k):
        there = lax.rem(dp + 8 - k, 8)
        return pltpu.make_async_remote_copy(
            src_ref=dtab.at[z_low, there], dst_ref=dtab.at[z_low, there], send_sem=t1_send.at[k - 1], recv_sem=t1_recv.at[k - 1],
            device_id=at(dp_=lax.rem(dp + k, 8)), device_id_type=MESH,
        )

    def t2(tab, slot, k):
        return pltpu.make_async_remote_copy(
            src_ref=tab.at[slot], dst_ref=tab.at[slot], send_sem=t2_send.at[k - 1], recv_sem=t2_recv.at[k - 1],
            device_id=at(z_=lax.rem(z + k, 4)), device_id_type=MESH,
        )

    def t3(k):
        return pltpu.make_async_remote_copy(
            src_ref=pieces.at[k], dst_ref=pieces.at[4], send_sem=t3_send.at[k], recv_sem=t3_recv.at[0], device_id=at(pipe_=k), device_id_type=MESH
        )

    @pl.when(pipe < 3)
    def _():
        t3(0).wait_recv()

    @pl.when(pipe == 3)
    def _():
        acc[0:8, :] = jnp.zeros((8, D), F32)

        @pl.loop(0, 16)
        def _(r):
            rows = pl.ds(pl.multiple_of(r * 32, 32), 32)
            keep = lax.broadcasted_iota(jnp.int32, (32, 1), 0) + r * 32 < length
            x = jnp.where(keep, hout[rows, :].astype(F32), 0.0)
            acc[0:8, :] += x[0:8] + x[8:16] + x[16:24] + x[24:32]

        pooled = jnp.sum(acc[0:8, :], axis=0, keepdims=True) / length.astype(F32)
        emb = pooled * lax.rsqrt(jnp.sum(pooled * pooled, axis=-1, keepdims=True) + 1e-6)
        emb = emb.astype(BF).astype(F32)

        @pl.when(z < 2)
        def _():
            for k in range(8):
                qtab[z_low, k : k + 1, :] = emb[:, k * 128 : (k + 1) * 128]

        @pl.when(z >= 2)
        def _():
            for k in range(8):
                dtab[z_low, dp, k : k + 1, :] = emb[:, k * 128 : (k + 1) * 128]
            for k in range(1, 8):
                t1(k).start()
            for k in range(1, 8):
                t1_in(k).wait_recv()
            for k in range(1, 4):
                t2(dtab, z_low, k).start()

        @pl.when(z < 2)
        def _():
            for k in range(1, 4):
                t2(qtab, z_low, k).start()

        for k in range(1, 4):
            there = lax.rem(z + 4 - k, 4)

            @pl.when(there < 2)
            def _():
                t2(qtab, lax.rem(there, 2), k).wait_recv()

            @pl.when(there >= 2)
            def _():
                t2(dtab, lax.rem(there, 2), k).wait_recv()

        doc_dp = lax.broadcasted_iota(jnp.int32, (8, 1), 0)
        losses = []
        for i in range(2):
            total, positive = jnp.zeros((1, 1), F32), jnp.zeros((1, 1), F32)
            for s in range(2):
                prod = dtab[s] * qtab[i][None]
                score = jnp.sum(jnp.sum(prod, axis=1), axis=1, keepdims=True) / 0.05
                total += jnp.sum(jnp.exp(score), axis=0, keepdims=True)
                hit = (doc_dp == dp) & (order[0, i] == s)
                positive += jnp.sum(jnp.where(hit, score, 0.0), axis=0, keepdims=True)
            losses.append(jnp.broadcast_to(jnp.log(total) - positive, (1, 128)))
        for k in (0, 1, 2, 3):
            row = 2 * k + z // 2
            pieces[k, 6:8, :] = jnp.zeros((2, 128), F32)
            for i in range(2):
                for at_row, line in ((i, qtab[i, pl.ds(row, 1), :]), (2 + i, dtab[i, dp, pl.ds(row, 1), :])):
                    pieces[k, at_row : at_row + 1, :] = jnp.where(z_low == 0, line, pltpu.roll(line, 64, 1))
                pieces[k, 4 + i : 5 + i, :] = losses[i]
            if k < 3:
                t3(k).start()
        pieces[4] = pieces[3]

    out[...] = pieces[4]

    for table in (hop1, hop2, yhop1, yhop2, d2d):
        for key, copy in table.items():
            if key[0] != "qkv":
                copy.wait_send()

    @pl.when(first == 0)
    def _():
        for table in (hop1, hop2, d2d):
            for key, copy in table.items():
                if key[0] == "qkv":
                    copy.wait_send()

    @pl.when(first == 1)
    def _():
        for copy in (*share[1], *share[2], *share[3], *share_on):
            copy.wait_send()

    sent()

    @pl.when(pipe == 3)
    def _():
        for k in range(3):
            t3(k).wait_send()

        @pl.when(z >= 2)
        def _():
            for k in range(1, 8):
                t1(k).wait_send()
            for k in range(1, 4):
                t2(dtab, z_low, k).wait_send()

        @pl.when(z < 2)
        def _():
            for k in range(1, 4):
                t2(qtab, z_low, k).wait_send()


def split(tile, out_q, out_d, out_loss):
    out_q[...] = tile[0:2, :64].astype(BF)
    out_d[...] = tile[2:4, :64].astype(BF)
    for i in range(2):
        out_loss[i] = tile[4 + i, 0]


def per_device(query_states, doc_states, query_len, doc_len, doc_order, w_qkv, w_out, w_up, w_down, gain_attn, gain_mlp):
    anyspace = pl.BlockSpec(memory_space=pl.ANY)
    smem = pl.BlockSpec(memory_space=pltpu.SMEM)
    vmem = pl.BlockSpec(memory_space=pltpu.VMEM)
    out = pl.pallas_call(
        kernel,
        out_shape=jax.ShapeDtypeStruct((8, 128), F32),
        in_specs=[anyspace, anyspace, smem, smem, smem, *[anyspace] * 6],
        out_specs=vmem,
        scratch_shapes=[
            pltpu.VMEM((4, 3, D, G), BF),
            pltpu.VMEM((4, G, D), BF),
            pltpu.VMEM((4, D, D), BF),
            pltpu.VMEM((4, D, D), BF),
            pltpu.VMEM((4, S, D), BF),
            pltpu.VMEM((S, D), BF),
            pltpu.VMEM((4, 3, S, G), BF),
            pltpu.VMEM((2, 4, 256, G), BF),
            pltpu.VMEM((2, 4, G, S), BF),
            pltpu.VMEM((4, G, S), BF),
            pltpu.VMEM((2, 4, S, G), BF),
            pltpu.VMEM((2, 256, G), F32),
            pltpu.VMEM((2, 256, G), F32),
            pltpu.VMEM((8, S, G), BF),
            pltpu.VMEM((2, 256, G), BF),
            pltpu.VMEM((2 * (HALF - DIRECT), D), BF),
            pltpu.VMEM((S, D), F32),
            pltpu.VMEM((S, D), BF),
            pltpu.VMEM((S, D), BF),
            pltpu.VMEM((2, 8, 128), F32),
            pltpu.VMEM((2, 8, 8, 128), F32),
            pltpu.VMEM((5, 8, 128), F32),
            pltpu.VMEM((16, D), F32),
            pltpu.SemaphoreType.DMA((N_SEMS,)),
            pltpu.SemaphoreType.DMA((N_SEMS,)),
            pltpu.SemaphoreType.DMA((12,)),
            pltpu.SemaphoreType.DMA((6,)),
            pltpu.SemaphoreType.DMA((6,)),
            pltpu.SemaphoreType.DMA((S // HALF,)),
            pltpu.SemaphoreType.DMA((S // HALF,)),
            pltpu.SemaphoreType.DMA((4,)),
            pltpu.SemaphoreType.DMA((4,)),
            pltpu.SemaphoreType.DMA((7,)),
            pltpu.SemaphoreType.DMA((7,)),
            pltpu.SemaphoreType.DMA((3,)),
            pltpu.SemaphoreType.DMA((3,)),
            pltpu.SemaphoreType.DMA((3,)),
            pltpu.SemaphoreType.DMA((1,)),
        ],
        compiler_params=pltpu.CompilerParams(collective_id=0, has_side_effects=True, vmem_limit_bytes=63 * 2**20),
        name="encode",
    )(query_states, doc_states, query_len, doc_len, doc_order, w_qkv, w_out, w_up, w_down, gain_attn, gain_mlp)
    return pl.pallas_call(
        split,
        out_shape=(jax.ShapeDtypeStruct((2, 64), BF), jax.ShapeDtypeStruct((2, 64), BF), jax.ShapeDtypeStruct((2,), F32)),
        in_specs=[vmem],
        out_specs=(vmem, vmem, smem),
        name="split",
    )(out)


def solution(mesh):
    in_specs = (
        P("dp", None, None),
        P("dp", None, None),
        P("dp"),
        P("dp"),
        P("dp", None),
        P("pipe", None, None, "tensor"),
        P("pipe", "tensor", None),
        P("pipe", None, "tensor"),
        P("pipe", "tensor", None),
        P("pipe", None),
        P("pipe", None),
    )
    out_specs = (P("dp", ("pipe", "tensor")), P("dp", ("pipe", "tensor")), P("dp"))
    return jax.shard_map(per_device, mesh=mesh, in_specs=in_specs, out_specs=out_specs, check_vma=False)
```
